128 devices in a mesh: blk: 64 (over z, y_lo, x, core), dp: 2 (over y_hi).
Axes of the slice: x: 4, y: 4 (y_hi: 2, y_lo: 2; y = y_hi * 2 + y_lo), z: 4, core: 2. Of those that a mesh axis runs over, the one named last changes fastest.
Arguments:
- inputs: bfloat16 [16384, 1024], P(('blk', 'dp')), may hold values from -6 to 6
- cotangent: bfloat16 [16384, 1024], P(('blk', 'dp')), may hold values from -2.5 to 2.5
- task_ids: int32 [16384], P(('blk', 'dp')), may hold values from 0 to 3
- group_counts: int32 [128, 8], P(('blk', 'dp')), may hold values from 1 to 16, as said below
- task_gate: float32 [4, 64], replicated, may hold values from 0.25 to 2
- w_in: bfloat16 [64, 1024, 2048], P('blk'), may hold values from -0.1875 to 0.1875
- w_out: bfloat16 [64, 2048, 1024], P('blk'), may hold values from -0.125 to 0.125
Outputs:
- input_grad: float32 [16384, 1024], P(('blk', 'dp'))
- grad_in: float32 [64, 1024, 2048], P('blk', 'dp')
- grad_out: float32 [64, 2048, 1024], P('blk', 'dp')
The draws below stay inside these ranges and needn't reach their ends.
Inputs may be any that keep to these rules, and one draw needn't show every extreme that they name: `group_counts`: in every draw one group has all 16 slots live on every device; the others vary from device to device.
All inputs are finite; a program needn't handle non-finite values.
Results may differ from the reference program's by a relative error of at most 0.0042.
Values may be sent and summed in bfloat16 or wider, within the bound.
A program may use at most 128 MiB of HBM per device.

```python
import math
import jax
import jax.numpy as jnp
from jax import lax

D = 1024
HW = 2048
GROUPS = 8
TASKS = 4
CAP = 16
EXPERTS = 64
SOURCES = 128
SAMPLES = 16384


def draw_group_counts(key, part):
    key_level = jax.random.fold_in(key, 11)
    key_raw = jax.random.fold_in(key, 12)
    key_full = jax.random.fold_in(key, 13)
    level = jax.random.randint(key_level, (GROUPS,), max(1, CAP // 4), CAP + 1)
    raw_values = jax.random.randint(key_raw, (SOURCES, GROUPS), 0, 1 << 20)
    counts = 1 + raw_values % level[None, :]
    full_group = jax.random.randint(key_full, (), 0, GROUPS)
    filled = jnp.where(jnp.arange(GROUPS)[None, :] == full_group, CAP, counts)
    return filled.astype(jnp.int32)


def with_ends(entries, rng, smallest, high):
    longest = entries.shape.index(max(entries.shape))
    spots = []
    for shift in (0, 1):
        where = [jax.random.randint(jax.random.fold_in(rng, axis), (), 0, length) for axis, length in enumerate(entries.shape)]
        where[longest] = (where[longest] + shift) % entries.shape[longest]
        spots.append(tuple(where))
    return entries.at[spots[0]].set(smallest).at[spots[1]].set(high)


def level_of(stream_key, dims, cuts, least, high):
    loudness = 1.0
    for dim, shards_of in cuts:
        steps = jax.random.uniform(jax.random.fold_in(jax.random.fold_in(stream_key, 6), dim), (shards_of,), jnp.float32, least / len(cuts), high / len(cuts))
        loudness = loudness * jnp.repeat(jnp.exp(steps), dims[dim] // shards_of).reshape((-1,) + (1,) * (len(dims) - 1 - dim))
    return loudness


def noise(key, dims, deviation, limit, shards=(), kind=jnp.bfloat16):
    level = level_of(key, dims, shards, -0.22, 0.18) if shards else 1.0
    drawn = jax.random.normal(key, dims, jnp.float32) * deviation * level
    return jnp.minimum(jnp.maximum(drawn, -limit), limit).astype(kind)


def setup_inputs(seed: int = 0) -> dict:
    key_list = jax.random.split(jax.random.key(seed), 8)
    return {
        "inputs": noise(key_list[0], (SAMPLES, D), 1.0, 6.0, ((0, 128),)),
        "cotangent": noise(key_list[1], (SAMPLES, D), 0.35, 2.5, ((0, 128),)),
        "task_ids": with_ends(jax.random.randint(key_list[2], (SAMPLES,), 0, TASKS), jax.random.fold_in(key_list[2], 1), 0, TASKS - 1).astype(jnp.int32),
        "group_counts": draw_group_counts(jax.random.fold_in(key_list[7], 71), 0),
        "task_gate": jnp.clip(jnp.exp(jax.random.uniform(key_list[4], (TASKS, EXPERTS), jnp.float32, math.log(0.25), math.log(2.0))), 0.25, 2.0),
        "w_in": noise(key_list[5], (EXPERTS, D, HW), D ** -0.5, 0.1875, ((0, 64),)),
        "w_out": noise(key_list[6], (EXPERTS, HW, D), HW ** -0.5, 0.125, ((0, 64),)),
    }


grad_scale = 0.0625


def reference(inputs, cotangent, task_ids, group_counts, task_gate, w_in, w_out):
    inputs_four = inputs.reshape(SOURCES, GROUPS, CAP, D)
    cot_four = cotangent.reshape(SOURCES, GROUPS, CAP, D)
    task_three = task_ids.reshape(SOURCES, GROUPS, CAP)
    slot_index = jnp.arange(CAP, dtype=jnp.int32)
    live_three = slot_index[None, None, :] < group_counts[:, :, None]

    def per_expert(accum, expert):
        group = (expert % GROUPS).astype(jnp.int32)
        x_rows = lax.dynamic_index_in_dim(inputs_four, group, 1, keepdims=False).reshape(SOURCES * CAP, D)
        cot_rows = lax.dynamic_index_in_dim(cot_four, group, 1, keepdims=False).reshape(SOURCES * CAP, D)
        task_rows = lax.dynamic_index_in_dim(task_three, group, 1, keepdims=False).reshape(SOURCES * CAP)
        live_rows = lax.dynamic_index_in_dim(live_three, group, 1, keepdims=False).reshape(SOURCES * CAP)
        column = lax.dynamic_index_in_dim(task_gate, expert.astype(jnp.int32), 1, keepdims=False)
        row_gate = jnp.where(live_rows, column[task_rows], jnp.zeros((), task_gate.dtype)).astype(jnp.float32)
        first_weight = lax.dynamic_index_in_dim(w_in, expert.astype(jnp.int32), 0, keepdims=False)
        second_weight = lax.dynamic_index_in_dim(w_out, expert.astype(jnp.int32), 0, keepdims=False)
        pre_act = jnp.dot(x_rows, first_weight, preferred_element_type=jnp.float32)
        sigmoid_act = jax.nn.sigmoid(pre_act)
        hidden = (pre_act * sigmoid_act).astype(jnp.bfloat16)
        scaled_cot = (row_gate[:, None] * cot_rows.astype(jnp.float32)).astype(jnp.bfloat16)
        hidden_cot = jnp.dot(scaled_cot, second_weight.T, preferred_element_type=jnp.float32)
        pre_cot = (hidden_cot * sigmoid_act * (1.0 + pre_act * (1.0 - sigmoid_act))).astype(jnp.bfloat16)
        grad_second = jnp.dot(hidden.T, scaled_cot, preferred_element_type=jnp.float32) * grad_scale
        grad_first = jnp.dot(x_rows.T, pre_cot, preferred_element_type=jnp.float32) * grad_scale
        row_grad = jnp.dot(pre_cot, first_weight.T, preferred_element_type=jnp.float32)
        current = lax.dynamic_index_in_dim(accum, group, 1, keepdims=False)
        accum = lax.dynamic_update_index_in_dim(accum, current + row_grad.reshape(SOURCES, CAP, D), group, 1)
        return accum, (grad_first, grad_second)

    start = jnp.zeros((SOURCES, GROUPS, CAP, D), jnp.float32)
    accum, stacked = lax.scan(per_expert, start, jnp.arange(EXPERTS, dtype=jnp.int32))
    return accum.reshape(SAMPLES, D), stacked[0], stacked[1]
```

```python
import jax
import jax.numpy as jnp
import numpy as np
from jax import lax
from jax.sharding import Mesh, PartitionSpec as P

grad_scale = 0.0625
LINE = ("x", "core")
PLANE = ("z", "ylo", "yhi")


def silu_parts(pre_act):
    sig = jax.nn.sigmoid(pre_act)
    return pre_act * sig, sig * (1.0 + pre_act * (1.0 - sig))


def on_device(inputs, cotangent, task_ids, group_counts, task_gate, w_in, w_out):
    groups = group_counts.shape[1]
    width = inputs.shape[1]
    cap = inputs.shape[0] // groups
    tasks = task_gate.shape[0]
    expert = (lax.axis_index("z") * lax.axis_size("ylo") + lax.axis_index("ylo")) * groups + lax.axis_index(
        "x"
    ) * lax.axis_size("core") + lax.axis_index("core")
    half = lax.axis_index("yhi")
    w1, w2 = w_in[0], w_out[0]
    hidden = w1.shape[1]
    match = jnp.arange(task_gate.shape[1], dtype=jnp.int32) == expert
    gate_column = jnp.sum(jnp.where(match[None, :], task_gate, 0.0), axis=1)
    live = jnp.arange(cap, dtype=jnp.int32)[None, :] < group_counts[0][:, None]
    tags = jnp.where(live, task_ids.reshape(groups, cap), tasks)
    both = jnp.concatenate([inputs, cotangent], axis=1).reshape(groups, cap, 2 * width)
    both = lax.all_to_all(both, LINE, split_axis=0, concat_axis=0, tiled=True)
    tags = lax.all_to_all(tags, LINE, split_axis=0, concat_axis=0, tiled=True)
    rows = lax.all_gather(both.reshape(groups * cap, 2 * width), PLANE, axis=0, tiled=False)
    tags = lax.all_gather(tags.reshape(groups * cap), PLANE, axis=0, tiled=False)
    nodes = rows.shape[0]
    count = nodes * groups * cap
    own = groups * cap
    x = rows[:, :, :width].reshape(count, width)
    cot = rows[:, :, width:].reshape(count, width)
    tags = tags.reshape(count)
    gate = jnp.sum(
        jnp.where(tags[:, None] == jnp.arange(tasks, dtype=jnp.int32)[None, :], gate_column[None, :], 0.0), axis=1
    )
    pre = jnp.dot(x, w1, preferred_element_type=jnp.float32)
    act, slope = silu_parts(pre)
    act = act.astype(jnp.bfloat16)
    scaled = (gate[:, None] * cot.astype(jnp.float32)).astype(jnp.bfloat16)
    back = lax.dot_general(scaled, w2, (((1,), (1,)), ((), ())), preferred_element_type=jnp.float32)
    pre_grad = (back * slope).astype(jnp.bfloat16)
    left1 = lax.dynamic_slice_in_dim(x, half * (width // 2), width // 2, 1)
    left2 = lax.dynamic_slice_in_dim(act, half * (hidden // 2), hidden // 2, 1)
    grad_out = lax.dot_general(left2, scaled, (((0,), (0,)), ((), ())), preferred_element_type=jnp.float32)
    grad_in = lax.dot_general(left1, pre_grad, (((0,), (0,)), ((), ())), preferred_element_type=jnp.float32)
    own_pre = pre_grad.reshape(nodes // 2, 2, own, hidden)
    own_pre = lax.dynamic_index_in_dim(own_pre, half, 1, keepdims=False)
    row_grad = lax.dot_general(
        own_pre.reshape(nodes // 2 * own, hidden), w1, (((1,), (1,)), ((), ())), preferred_element_type=jnp.float32
    )
    row_grad = row_grad.reshape(nodes // 2, own, width).astype(jnp.bfloat16)
    row_grad = lax.all_to_all(row_grad, ("z", "ylo"), split_axis=0, concat_axis=0, tiled=True)
    row_grad = jnp.sum(row_grad.astype(jnp.float32), axis=0).astype(jnp.bfloat16)
    home = lax.all_to_all(row_grad.reshape(groups, cap, width), LINE, split_axis=0, concat_axis=0, tiled=True)
    return (
        home.astype(jnp.float32).reshape(groups * cap, width),
        (grad_in * grad_scale)[None],
        (grad_out * grad_scale)[None],
    )


def solution(mesh):
    fine = Mesh(mesh.devices.reshape(4, 2, 4, 2, 2), ("z", "ylo", "x", "core", "yhi"))
    blk = ("z", "ylo", "x", "core")
    every = blk + ("yhi",)
    in_specs = (P(every, None), P(every, None), P(every), P(every, None), P(), P(blk, None, None), P(blk, None, None))
    out_specs = (P(every, None), P(blk, "yhi", None), P(blk, "yhi", None))
    return jax.shard_map(on_device, mesh=fine, in_specs=in_specs, out_specs=out_specs, check_vma=False)
```

```python
import jax
import jax.numpy as jnp
from jax import lax
from jax.experimental import pallas as pl
from jax.experimental.pallas import tpu as pltpu
from jax.sharding import PartitionSpec as P

MESH = pl.DeviceIdType.MESH
F32, BF16 = jnp.float32, jnp.bfloat16
grad_scale = 0.0625

RING = 4
LINE = 8
CAP = 16
HALF = LINE * CAP // 2
PART = HALF // 2
CHUNK = 4
ROWS = CHUNK * HALF
PAIR = 2 * ROWS
NT = 512

A, B = 0, 1
ORDER = (
    (A, 0, 0), (B, 0, 0), (B, 0, 1), (B, 0, 3),
    (A, 0, 1), (A, 0, 3), (A, 1, 0), (B, 3, 0),
    (A, 1, 1), (A, 1, 3), (B, 3, 1), (B, 0, 2),
    (A, 3, 0), (A, 2, 0), (B, 1, 0), (B, 1, 1),
    (A, 0, 2), (A, 1, 2), (B, 3, 3), (B, 3, 2),
    (A, 3, 1), (A, 3, 3), (B, 1, 3), (B, 1, 2),
    (A, 2, 1), (A, 2, 3), (B, 2, 0), (B, 2, 1),
    (A, 3, 2), (A, 2, 2), (B, 2, 3), (B, 2, 2),
)
SLOT = {key: n for n, key in enumerate(ORDER)}
RS_CHUNK = {0: 0, 1: 1, 2: 2, 4: 3}
RS_SLOT = {key: RS_CHUNK[n // CHUNK] * CHUNK + n % CHUNK for key, n in SLOT.items() if n // CHUNK in RS_CHUNK}


def hops():
    table = {}

    def add(name, axis, half, dy, dz, split):
        for sign in (1, -1):
            if split:
                if axis == "y":
                    dy_s, dz_s = (-sign * dy) % RING, dz
                else:
                    dy_s, dz_s = dy, (-sign * dz) % RING
                part = 0 if sign == 1 else 1
            else:
                dy_s, dz_s, part = dy, dz, None
            there = (half, (dy_s - sign) % RING, dz_s) if axis == "y" else (half, dy_s, (dz_s - sign) % RING)
            table.setdefault(name, []).append((axis, sign, (half, dy_s, dz_s), part, there))

    add("y1", "y", A, 0, 0, False)
    add("y2", "y", B, 0, 0, False)
    add("y3", "y", A, 1, 0, True)
    add("y4", "y", B, 0, 1, False)
    add("y5", "y", B, 0, 3, False)
    add("y6", "y", B, 0, 2, False)
    add("y7", "y", B, 1, 0, True)
    add("y8", "y", B, 1, 1, True)
    add("y9", "y", B, 1, 3, True)
    add("y10", "y", B, 1, 2, True)
    add("z1", "z", B, 0, 0, False)
    add("z2", "z", A, 0, 0, False)
    add("z3", "z", B, 0, 1, True)
    add("z4", "z", A, 1, 0, False)
    add("z7", "z", A, 3, 0, False)
    add("z5", "z", A, 0, 1, True)
    add("z6", "z", A, 1, 1, True)
    add("z8", "z", A, 2, 0, False)
    add("z9", "z", A, 3, 1, True)
    add("z10", "z", A, 2, 1, True)
    return table


HOPS = hops()
HOP_SEM = {name: 2 * n for n, name in enumerate(HOPS)}


def kernel(
    x_hbm, cot_hbm, tag_hbm, gate_smem, w1_hbm, w2_hbm,
    home_hbm, gin_hbm, gout_hbm,
    rows, w1, w2, w1t, w2t, sc, act, pg, xt, actt, gin, gout, gates, tag_line, tag_all,
    rgb, ys, ry, zs, zq, zr, fs, home, home32,
    local_sem, tagp_sem, tagp_send, line_sem, line_send, tag_sem, tag_send, slot_sem, hop_send,
    ry_sem, ry_send, zq_sem, zq_send, zr_sem, zr_send, home_sem, home_send, out_sem,
):
    blk, yhi = lax.axis_index("blk"), lax.axis_index("dp")
    c = blk % 2
    x = (blk // 2) % RING
    y = yhi * 2 + (blk // LINE) % 2
    z = blk // (2 * LINE)
    me = x * 2 + c

    def on_line(j):
        return ((z * 2 + y % 2) * LINE + j, yhi)

    def on_plane(dy, dz):
        ty, tz = (y + dy) % RING, (z + dz) % RING
        return ((tz * 2 + ty % 2) * LINE + me, ty // 2)

    def weight_copy(n):
        return pltpu.make_async_copy((w1_hbm, w2_hbm)[n], (w1, w2)[n], local_sem.at[n])

    def line_copies(step):
        j = (me + step) % LINE
        here = pl.ds(pl.multiple_of(j * CAP, CAP), CAP)
        slot = me // CHUNK
        there = pl.ds(pl.multiple_of((me % CHUNK) * CAP, CAP), CAP)
        out = []
        for kind, src in ((0, x_hbm), (1, cot_hbm)):
            out.append((src.at[here], rows.at[slot, kind, there], line_sem.at[me, kind], line_send.at[step, kind], j))
        return (tag_hbm.at[j], tag_line.at[me], tagp_sem.at[me], tagp_send.at[step], j), out

    def remote(src, dst, recv, send, device):
        return pltpu.make_async_remote_copy(
            src_ref=src, dst_ref=dst, send_sem=send, recv_sem=recv, device_id=device, device_id_type=MESH
        )

    def line_remote(spec):
        src, dst, recv, send, j = spec
        return remote(src, dst, recv, send, on_line(j))

    def hop_copy(name, n):
        axis, sign, here, part, there = HOPS[name][n]
        src, dst = rows.at[SLOT[here]], rows.at[SLOT[there]]
        if part is not None:
            span = pl.ds(part * PART, PART)
            src, dst = rows.at[SLOT[here], :, span], rows.at[SLOT[there], :, span]
        device = on_plane(sign, 0) if axis == "y" else on_plane(0, sign)
        return remote(src, dst, slot_sem.at[SLOT[there]], hop_send.at[HOP_SEM[name] + n], device)

    def send_hops(*names):
        for name in names:
            for n in range(2):
                hop_copy(name, n).start()

    def wait_slots(*keys):
        for key in keys:
            n = SLOT[key]
            pltpu.make_async_copy(rows.at[n], rows.at[n], slot_sem.at[n]).wait()

    def y_copy(half, dz):
        return remote(
            ys.at[half, dz], ry.at[half, dz], ry_sem.at[half, dz], ry_send.at[half, dz], on_plane(1 if half == A else 3, 0)
        )

    def y_send(*keys):
        for half, dz in keys:
            ys[half, dz] = rgb[RS_SLOT[(half, 1 if half == A else 3, dz)]].astype(BF16)
        for half, dz in keys:
            y_copy(half, dz).start()

    def relay_copy(half):
        return remote(zs.at[half, 0], zq.at[half], zq_sem.at[half], zq_send.at[half], on_plane(0, 1 if half == A else 3))

    def z_copy(half, dz):
        n = 0 if dz == 1 else 1
        return remote(zs.at[half, 1 + n], zr.at[half, n], zr_sem.at[half, n], zr_send.at[half, n], on_plane(0, dz))

    def total(half, dz):
        pltpu.make_async_copy(ry.at[half, dz], ry.at[half, dz], ry_sem.at[half, dz]).wait()
        return rgb[RS_SLOT[(half, 0, dz)]] + ry[half, dz].astype(F32)

    def transpose_weights():
        def body(i, _):
            cols = pl.ds(pl.multiple_of(i * 256, 256), 256)
            w2t[:, cols] = w2[cols, :].T
            w1t[cols, :] = w1[:, cols].T
            return 0

        lax.fori_loop(0, w1.shape[1] // 256, body, 0)

    def make_gates():
        row = lax.broadcasted_iota(jnp.int32, (HALF, 128), 0)
        lane = lax.broadcasted_iota(jnp.int32, (HALF, 128), 1)
        for n, (half, dy, dz) in enumerate(ORDER):
            tags = tag_all[dy * RING + dz][0:1, :]
            lanes = jnp.zeros_like(tags)
            for task in range(4):
                lanes = jnp.where(tags == float(task), gate_smem[0, task], lanes)
            picked = jnp.where(lane == row + half * HALF, jnp.broadcast_to(lanes, (HALF, 128)), 0.0)
            gates[n] = jnp.broadcast_to(jnp.sum(picked, axis=1, keepdims=True), (HALF, 128))

    def forward(k):
        four = pl.ds(k * CHUNK, CHUNK)
        span = pl.ds(pl.multiple_of((k % 2) * ROWS, ROWS), ROWS)
        gate = gates[four].reshape(ROWS, 128)
        for n in range(rows.shape[3] // 128):
            cols = pl.ds(n * 128, 128)
            cot = rows[four, 1, :, cols].reshape(ROWS, 128).astype(F32)
            sc[span, cols] = (gate * cot).astype(BF16)

        def body(n, _):
            cols = pl.ds(pl.multiple_of(n * NT, NT), NT)
            pre = jnp.dot(rows[four, 0].reshape(ROWS, rows.shape[3]), w1[:, cols], preferred_element_type=F32)
            back = jnp.dot(sc[span, :], w2t[:, cols], preferred_element_type=F32)
            sig = 0.5 * jnp.tanh(0.5 * pre) + 0.5
            value = pre * sig
            act[span, cols] = value.astype(BF16)
            pg[span, cols] = (back * (sig + value * (1.0 - sig))).astype(BF16)
            return 0

        lax.fori_loop(0, w1.shape[1] // NT, body, 0)

    def row_grads(k, r):
        span = pl.ds(pl.multiple_of((k % 2) * ROWS, ROWS), ROWS)

        def body(n, _):
            cols = pl.ds(pl.multiple_of(n * NT, NT), NT)
            part = jnp.dot(pg[span, :], w1t[:, cols], preferred_element_type=F32)
            rgb[pl.ds(r * CHUNK, CHUNK), :, cols] = part.reshape(CHUNK, HALF, NT)
            return 0

        lax.fori_loop(0, w1t.shape[1] // NT, body, 0)

    def turn(k):
        eight = pl.ds((k - 1) * CHUNK, 2 * CHUNK)
        width = xt.shape[0]
        for n in range(width // 256):
            cols = pl.ds(pl.multiple_of(yhi * width + n * 256, 256), 256)
            xt[pl.ds(n * 256, 256), :] = rows[eight, 0, :, cols].reshape(PAIR, 256).T
        width = actt.shape[0]
        for n in range(width // 256):
            cols = pl.ds(pl.multiple_of(yhi * width + n * 256, 256), 256)
            actt[pl.ds(n * 256, 256), :] = act[:, cols].T

    def grads():
        def body_in(n, _):
            cols = pl.ds(pl.multiple_of(n * NT, NT), NT)
            gin[:, cols] += jnp.dot(xt[...], pg[:, cols], preferred_element_type=F32)
            return 0

        def body_out(n, _):
            cols = pl.ds(pl.multiple_of(n * 256, 256), 256)
            gout[:, cols] += jnp.dot(actt[...], sc[:, cols], preferred_element_type=F32)
            return 0

        lax.fori_loop(0, gin.shape[1] // NT, body_in, 0)
        lax.fori_loop(0, gout.shape[1] // 256, body_out, 0)

    def out_copy(which, n):
        acc, hbm = ((gin, gin_hbm), (gout, gout_hbm))[which]
        span = pl.ds(pl.multiple_of(n * 128, 128), 128)
        return pltpu.make_async_copy(acc.at[span], hbm.at[span], out_sem.at[which])

    def last_grads():
        def body_in(n, _):
            span = pl.ds(pl.multiple_of(n * 128, 128), 128)
            gin[span, :] = (gin[span, :] + jnp.dot(xt[span, :], pg[...], preferred_element_type=F32)) * grad_scale
            out_copy(0, n).start()
            return 0

        def body_out(n, _):
            span = pl.ds(pl.multiple_of(n * 128, 128), 128)
            gout[span, :] = (gout[span, :] + jnp.dot(actt[span, :], sc[...], preferred_element_type=F32)) * grad_scale
            out_copy(1, n).start()
            return 0

        lax.fori_loop(0, gin.shape[0] // 128, body_in, 0)
        lax.fori_loop(0, gout.shape[0] // 128, body_out, 0)

    for n in range(2):
        weight_copy(n).start()
    tag_own, own = line_copies(0)
    pltpu.make_async_copy(tag_own[0], tag_own[1], tag_own[2]).start()
    for spec in own:
        pltpu.make_async_copy(spec[0], spec[1], spec[2]).start()

    barrier = pltpu.get_barrier_semaphore()
    for step in range(1, LINE):
        pl.semaphore_signal(barrier, inc=1, device_id=on_line((me + step) % LINE), device_id_type=MESH)
    for dy in range(RING):
        for dz in range(RING):
            if dy or dz:
                pl.semaphore_signal(barrier, inc=1, device_id=on_plane(dy, dz), device_id_type=MESH)
    pl.semaphore_wait(barrier, LINE - 1 + RING * RING - 1)

    for step in range(1, LINE):
        line_remote(line_copies(step)[0]).start()
    for step in range(1, LINE):
        for spec in line_copies(step)[1]:
            line_remote(spec).start()

    gin[...] = jnp.zeros_like(gin)
    gout[...] = jnp.zeros_like(gout)

    for j in range(LINE):
        pltpu.make_async_copy(tag_line.at[j], tag_line.at[j], tagp_sem.at[j]).wait()
    tags = tag_line[0]
    for j in range(1, LINE):
        tags = tags + tag_line[j]
    tag_all[0] = tags

    def tag_copy(dy, dz):
        there = ((-dy) % RING) * RING + (-dz) % RING
        return remote(tag_all.at[0], tag_all.at[there], tag_sem, tag_send, on_plane(dy, dz))

    around = [(dy, dz) for dy in range(RING) for dz in range(RING) if dy or dz]
    for dy, dz in around:
        tag_copy(dy, dz).start()

    def wait_line(half):
        for j in range(half * CHUNK, half * CHUNK + CHUNK):
            for kind in range(2):
                part = rows.at[half, kind, pl.ds((j % CHUNK) * CAP, CAP)]
                pltpu.make_async_copy(part, part, line_sem.at[j, kind]).wait()

    wait_line(A)
    wait_line(B)
    send_hops("y1", "z1", "y2", "z2")

    for n in range(2):
        weight_copy(n).wait()
    transpose_weights()
    others = tag_all.at[pl.ds(1, RING * RING - 1)]
    pltpu.make_async_copy(others, others, tag_sem).wait()
    make_gates()

    def step(k, _):
        @pl.when(k == 0)
        def _():
            wait_slots((A, 1, 0), (A, 3, 0), (B, 0, 1), (B, 0, 3))
            send_hops("y3", "z3", "y4", "z4", "y5", "z7")

        @pl.when(k == 1)
        def _():
            wait_slots((B, 1, 0), (B, 3, 0), (A, 0, 1), (A, 0, 3))
            send_hops("z5")

        @pl.when(k == 2)
        def _():
            wait_slots((B, 1, 1), (B, 3, 1), (A, 1, 1), (A, 1, 3))
            send_hops("z6", "y8", "z8")

        @pl.when(k == 4)
        def _():
            wait_slots((B, 1, 2), (B, 3, 2), (A, 0, 2), (A, 1, 2))
            send_hops("y10")

        @pl.when(k == 6)
        def _():
            wait_slots((B, 2, 0), (B, 2, 1))

        @pl.when(k == 7)
        def _():
            wait_slots((A, 3, 2), (A, 2, 2), (B, 2, 3), (B, 2, 2))

        forward(k)

        @pl.when(k == 1)
        def _():
            wait_slots((A, 2, 0), (B, 0, 2))
            send_hops("y6", "y7")

        @pl.when(k == 3)
        def _():
            wait_slots((A, 3, 1), (A, 3, 3), (B, 1, 3), (B, 3, 3))
            send_hops("z9", "y9")

        @pl.when(k == 5)
        def _():
            wait_slots((A, 2, 1), (A, 2, 3))
            send_hops("z10")

        @pl.when(k == 6)
        def _():
            for half, dz in ((A, 1), (B, 3)):
                pltpu.make_async_copy(zq.at[half], zq.at[half], zq_sem.at[half]).wait()
                zs[half, 1 if dz == 1 else 2] = (total(half, dz) + zq[half].astype(F32)).astype(BF16)
            z_copy(A, 1).start()
            z_copy(B, 3).start()

        @pl.when(k == 7)
        def _():
            for half in (A, B):
                value = total(half, 0)
                for n in range(2):
                    pltpu.make_async_copy(zr.at[half, n], zr.at[half, n], zr_sem.at[half, n]).wait()
                    value = value + zr[half, n].astype(F32)
                fs[pl.ds(half * HALF, HALF), :] = value.astype(BF16)
            for n in range(LINE):
                home_copy(n).start() if n else home_local().start()

        @pl.when((k < 3) | (k == 4))
        def _():
            row_grads(k, k - k // 4)

        @pl.when(k == 1)
        def _():
            y_send((A, 0), (B, 0))

        @pl.when(k == 2)
        def _():
            y_send((A, 1), (A, 3), (B, 1))

        @pl.when(k == 4)
        def _():
            y_send((A, 2), (B, 2), (B, 3))

        @pl.when(k % 2 == 1)
        def _():
            turn(k)

            @pl.when(k < 7)
            def _():
                grads()

            @pl.when(k == 7)
            def _():
                last_grads()

        @pl.when(k == 3)
        def _():
            for half, dz in ((A, 3), (B, 1)):
                zs[half, 1 if dz == 1 else 2] = total(half, dz).astype(BF16)
            z_copy(A, 3).start()
            z_copy(B, 1).start()

        @pl.when(k == 5)
        def _():
            for half in (A, B):
                zs[half, 0] = total(half, 2).astype(BF16)
            for half in (A, B):
                relay_copy(half).start()

        return 0

    def home_copy(step):
        j = (me + step) % LINE
        return remote(
            fs.at[pl.ds(pl.multiple_of(j * CAP, CAP), CAP)],
            home.at[pl.ds(pl.multiple_of(me * CAP, CAP), CAP)],
            home_sem.at[me],
            home_send.at[step],
            on_line(j),
        )

    def home_local():
        span = pl.ds(pl.multiple_of(me * CAP, CAP), CAP)
        home[span, :] = fs[span, :]
        return home_nothing

    class home_nothing:
        start = staticmethod(lambda: None)

    lax.fori_loop(0, len(ORDER) // CHUNK, step, 0)

    for n in range(1, LINE):
        span = pl.ds(pl.multiple_of(((me + n) % LINE) * CAP, CAP), CAP)
        pltpu.make_async_copy(home.at[span], home.at[span], home_sem.at[(me + n) % LINE]).wait()
    home32[...] = home[...].astype(F32)
    pltpu.make_async_copy(home32, home_hbm, local_sem.at[2]).start()

    for step_n in range(1, LINE):
        tag_spec, specs = line_copies(step_n)
        line_remote(tag_spec).wait_send()
        for spec in specs:
            line_remote(spec).wait_send()
        home_copy(step_n).wait_send()
    pltpu.make_async_copy(others, others, tag_send).wait()
    for name in HOPS:
        for n in range(2):
            hop_copy(name, n).wait_send()
    for half in (A, B):
        for dz in range(RING):
            y_copy(half, dz).wait_send()
        relay_copy(half).wait_send()
        for dz in (1, 3):
            z_copy(half, dz).wait_send()
    pltpu.make_async_copy(home32, home_hbm, local_sem.at[2]).wait()
    pltpu.make_async_copy(gin, gin_hbm, out_sem.at[0]).wait()
    pltpu.make_async_copy(gout, gout_hbm, out_sem.at[1]).wait()


def on_device(inputs, cotangent, task_ids, group_counts, task_gate, w_in, w_out):
    groups = group_counts.shape[1]
    width = inputs.shape[1]
    hidden = w_in.shape[2]
    tasks = task_gate.shape[0]
    blk = lax.axis_index("blk")
    match = jnp.arange(task_gate.shape[1], dtype=jnp.int32) == blk
    gate_column = jnp.sum(jnp.where(match[None, :], task_gate, 0.0), axis=1).reshape(1, tasks)
    live = jnp.arange(CAP, dtype=jnp.int32)[None, :] < group_counts[0][:, None]
    tags = jnp.where(live, task_ids.reshape(groups, CAP), tasks).astype(F32)
    lane = jnp.arange(LINE * CAP, dtype=jnp.int32)
    tags = jnp.where((lane // CAP == blk % LINE)[None, :], jnp.tile(tags, (1, LINE)), 0.0)
    tags = jnp.broadcast_to(tags[:, None, :], (groups, 8, LINE * CAP))
    any_space = pl.BlockSpec(memory_space=pl.ANY)
    dma = pltpu.SemaphoreType.DMA
    home, gin, gout = pl.pallas_call(
        kernel,
        out_shape=(
            jax.ShapeDtypeStruct((groups * CAP, width), F32),
            jax.ShapeDtypeStruct((width // 2, hidden), F32),
            jax.ShapeDtypeStruct((hidden // 2, width), F32),
        ),
        in_specs=[any_space] * 3 + [pl.BlockSpec(memory_space=pltpu.SMEM)] + [any_space] * 2,
        out_specs=(any_space,) * 3,
        scratch_shapes=[
            pltpu.VMEM((len(ORDER), 2, HALF, width), BF16),
            pltpu.VMEM((width, hidden), BF16),
            pltpu.VMEM((hidden, width), BF16),
            pltpu.VMEM((hidden, width), BF16),
            pltpu.VMEM((width, hidden), BF16),
            pltpu.VMEM((PAIR, width), BF16),
            pltpu.VMEM((PAIR, hidden), BF16),
            pltpu.VMEM((PAIR, hidden), BF16),
            pltpu.VMEM((width // 2, PAIR), BF16),
            pltpu.VMEM((hidden // 2, PAIR), BF16),
            pltpu.VMEM((width // 2, hidden), F32),
            pltpu.VMEM((hidden // 2, width), F32),
            pltpu.VMEM((len(ORDER), HALF, 128), F32),
            pltpu.VMEM((LINE, 8, LINE * CAP), F32),
            pltpu.VMEM((RING * RING, 8, LINE * CAP), F32),
            pltpu.VMEM((16, HALF, width), F32),
            pltpu.VMEM((2, RING, HALF, width), BF16),
            pltpu.VMEM((2, RING, HALF, width), BF16),
            pltpu.VMEM((2, 3, HALF, width), BF16),
            pltpu.VMEM((2, HALF, width), BF16),
            pltpu.VMEM((2, 2, HALF, width), BF16),
            pltpu.VMEM((2 * HALF, width), BF16),
            pltpu.VMEM((2 * HALF, width), BF16),
            pltpu.VMEM((2 * HALF, width), F32),
            dma((3,)),
            dma((LINE,)),
            dma((LINE,)),
            dma((LINE, 2)),
            dma((LINE, 2)),
            dma(()),
            dma(()),
            dma((len(ORDER),)),
            dma((2 * len(HOPS),)),
            dma((2, RING)),
            dma((2, RING)),
            dma((2,)),
            dma((2,)),
            dma((2, 2)),
            dma((2, 2)),
            dma((LINE,)),
            dma((LINE,)),
            dma((2,)),
        ],
        compiler_params=pltpu.CompilerParams(
            collective_id=0, has_side_effects=True, vmem_limit_bytes=63 * 1024 * 1024
        ),
    )(inputs, cotangent, tags, gate_column, w_in[0], w_out[0])
    return home, gin[None], gout[None]


def solution(mesh):
    in_specs = (
        P(("blk", "dp"), None),
        P(("blk", "dp"), None),
        P(("blk", "dp")),
        P(("blk", "dp"), None),
        P(),
        P("blk", None, None),
        P("blk", None, None),
    )
    out_specs = (P(("blk", "dp"), None), P("blk", "dp", None), P("blk", "dp", None))
    return jax.shard_map(on_device, mesh=mesh, in_specs=in_specs, out_specs=out_specs, check_vma=False)
```

```python
import jax
import jax.numpy as jnp
from jax import lax
from jax.experimental import pallas as pl
from jax.experimental.pallas import tpu as pltpu
from jax.sharding import PartitionSpec as P

MESH = pl.DeviceIdType.MESH
F32, BF16 = jnp.float32, jnp.bfloat16
grad_scale = 0.0625

RING = 4
LINE = 8
CAP = 16
HALF = LINE * CAP // 2
PART = HALF // 2
CHUNK = 4
ROWS = CHUNK * HALF
PAIR = 2 * ROWS
NT = 512
VMEM_LIMIT = 46 * 1024 * 1024

A, B = 0, 1
ORDER = (
    (A, 0, 0), (B, 0, 0), (A, 0, 1), (A, 0, 3),
    (A, 1, 0), (B, 0, 1), (B, 0, 3), (B, 3, 0),
    (A, 1, 1), (A, 1, 3), (B, 3, 1), (B, 0, 2),
    (A, 0, 2), (A, 1, 2), (B, 3, 3), (B, 3, 2),
    (A, 3, 0), (B, 1, 0), (B, 1, 1), (B, 1, 3),
    (A, 2, 0), (B, 1, 2), (A, 3, 1), (A, 3, 3),
    (A, 2, 1), (A, 2, 3), (B, 2, 0), (B, 2, 1),
    (A, 3, 2), (A, 2, 2), (B, 2, 3), (B, 2, 2),
)
SLOT = {key: n for n, key in enumerate(ORDER)}
OWED = 4


def place(r, q):
    return {0: 0, 1: 2, 3: 4, 2: 6}[r] + q


STEPS = ((0, 1), (1, 0), (3, 0), (1, 1), (3, 1), (2, 0), (2, 1))


def hops():
    table = {}

    def add(name, axis, half, dy, dz, split):
        for sign in (1, -1):
            if split:
                if axis == "y":
                    dy_s, dz_s = (-sign * dy) % RING, dz
                else:
                    dy_s, dz_s = dy, (-sign * dz) % RING
                part = 0 if sign == 1 else 1
            else:
                dy_s, dz_s, part = dy, dz, None
            there = (half, (dy_s - sign) % RING, dz_s) if axis == "y" else (half, dy_s, (dz_s - sign) % RING)
            table.setdefault(name, []).append((axis, sign, (half, dy_s, dz_s), part, there))

    add("y1", "y", A, 0, 0, False)
    add("y2", "y", B, 0, 0, False)
    add("y3", "y", A, 1, 0, True)
    add("y4", "y", B, 0, 1, False)
    add("y5", "y", B, 0, 3, False)
    add("y6", "y", B, 0, 2, False)
    add("y7", "y", B, 1, 0, True)
    add("y8", "y", B, 1, 1, True)
    add("y9", "y", B, 1, 3, True)
    add("y10", "y", B, 1, 2, True)
    add("z1", "z", B, 0, 0, False)
    add("z2", "z", A, 0, 0, False)
    add("z3", "z", B, 0, 1, True)
    add("z4", "z", A, 1, 0, False)
    add("z7", "z", A, 3, 0, False)
    add("z5", "z", A, 0, 1, True)
    add("z6", "z", A, 1, 1, True)
    add("z8", "z", A, 2, 0, False)
    add("z9", "z", A, 3, 1, True)
    add("z10", "z", A, 2, 1, True)
    return table


HOPS = hops()
HOP_SEM = {name: 2 * n for n, name in enumerate(HOPS)}


def kernel(
    x_hbm, cot_hbm, ids_ref, count_smem, gate_smem, w1_hbm, w2_hbm,
    home_ref, gin, gout,
    rows, w1, w2, w1t, w2t, sc, act, pg, xt, actt, gates, tag_out, tag_line, tag_all,
    rgb, ys, ry, zs, zq, zr, fs, home,
    local_sem, tagp_sem, tagp_send, line_sem, line_send, tag_sem, tag_send, slot_sem, hop_send,
    ry_sem, ry_send, zq_sem, zq_send, zr_sem, zr_send, home_sem, home_send,
):
    blk, yhi = lax.axis_index("blk"), lax.axis_index("dp")
    c = blk % 2
    x = (blk // 2) % RING
    y = yhi * 2 + (blk // LINE) % 2
    z = blk // (2 * LINE)
    me = x * 2 + c

    def line_index(dr, dq):
        return ((x + dr) % RING) * 2 + (c + dq) % 2

    def on_line(dr, dq):
        return ((z * 2 + y % 2) * LINE + line_index(dr, dq), yhi)

    def on_plane(dy, dz):
        ty, tz = (y + dy) % RING, (z + dz) % RING
        return ((tz * 2 + ty % 2) * LINE + me, ty // 2)

    def remote(src, dst, recv, send, device):
        return pltpu.make_async_remote_copy(
            src_ref=src, dst_ref=dst, send_sem=send, recv_sem=recv, device_id=device, device_id_type=MESH
        )

    def arrive(ref, sem):
        pltpu.make_async_copy(ref, ref, sem).wait()

    def weight_copy(n):
        return pltpu.make_async_copy((w1_hbm, w2_hbm)[n], (w1, w2)[n], local_sem.at[n])

    def cap_rows(j):
        return pl.ds(pl.multiple_of(j * CAP, CAP), CAP)

    def piece(n):
        return n // CHUNK, pl.ds((n % CHUNK) * CAP, CAP)

    def line_copies(dr, dq):
        there = place((-dr) % RING, dq)
        here = cap_rows(line_index(dr, dq))
        slot, span = piece(there)
        for kind, src in ((0, x_hbm), (1, cot_hbm)):
            if (dr, dq) == (0, 0):
                yield pltpu.make_async_copy(src.at[here], rows.at[slot, kind, span], line_sem.at[there])
            else:
                send = line_send.at[there, kind]
                yield remote(src.at[here], rows.at[slot, kind, span], line_sem.at[there], send, on_line(dr, dq))

    def tag_line_copy(dr, dq):
        there = place((-dr) % RING, dq)
        return remote(tag_out.at[there], tag_line.at[there], tagp_sem.at[there], tagp_send.at[there], on_line(dr, dq))

    def tag_copy(dy, dz):
        there = ((-dy) % RING) * RING + (-dz) % RING
        return remote(tag_all.at[0], tag_all.at[there], tag_sem, tag_send, on_plane(dy, dz))

    def hop_copy(name, n, span=None):
        axis, sign, here, part, there = HOPS[name][n]
        if part is not None:
            span = pl.ds(part * PART, PART)
        src, dst = rows.at[SLOT[here]], rows.at[SLOT[there]]
        if span is not None:
            src, dst = rows.at[SLOT[here], :, span], rows.at[SLOT[there], :, span]
        device = on_plane(sign, 0) if axis == "y" else on_plane(0, sign)
        return remote(src, dst, slot_sem.at[SLOT[there]], hop_send.at[HOP_SEM[name] + n], device)

    def send_hops(*names):
        for name in names:
            for n in range(2):
                hop_copy(name, n).start()

    def send_piece(n):
        half, span = piece(n)
        arrive(rows.at[half, :, span], line_sem.at[n])
        for name in (("y1", "z2"), ("y2", "z1"))[half]:
            for m in range(2):
                hop_copy(name, m, span).start()

    def wait_slots(*keys):
        for key in keys:
            arrive(rows.at[SLOT[key]], slot_sem.at[SLOT[key]])

    def y_copy(half, dz):
        device = on_plane(1 if half == A else 3, 0)
        return remote(ys.at[half, dz], ry.at[half, dz], ry_sem.at[half, dz], ry_send.at[half, dz], device)

    def y_send(*keys):
        for half, dz in keys:
            ys[half, dz] = rgb[SLOT[(half, 1 if half == A else 3, dz)]].astype(BF16)
        for half, dz in keys:
            y_copy(half, dz).start()

    def relay_copy(half):
        return remote(zs.at[half, 0], zq.at[half], zq_sem.at[half], zq_send.at[half], on_plane(0, 1 if half == A else 3))

    def z_copy(half, dz):
        n = 0 if dz == 1 else 1
        return remote(zs.at[half, 1 + n], zr.at[half, n], zr_sem.at[half, n], zr_send.at[half, n], on_plane(0, dz))

    def home_copy(dr, dq):
        n = place(dr, dq)
        there = place((-dr) % RING, dq)
        src = fs.at[pl.ds(n * CAP, CAP)]
        return remote(src, home.at[cap_rows(me)], home_sem.at[there], home_send.at[n], on_line(dr, dq))

    def total(half, dz):
        arrive(ry.at[half, dz], ry_sem.at[half, dz])
        return rgb[SLOT[(half, 0, dz)]] + ry[half, dz].astype(F32)

    def transpose_weights():
        def body(i, _):
            cols = pl.ds(pl.multiple_of(i * 256, 256), 256)
            w2t[:, cols] = w2[cols, :].T
            w1t[cols, :] = w1[:, cols].T
            return 0

        lax.fori_loop(0, w1.shape[1] // 256, body, 0)

    def make_tags():
        lane = lax.broadcasted_iota(jnp.int32, (8, 128), 1)
        count = jnp.zeros_like(lane)
        for group in range(LINE):
            count = jnp.where(lane // CAP == group, count_smem[0, group], count)
        tags = jnp.where(lane % CAP < count, jnp.broadcast_to(ids_ref[...], (8, 128)), 4).astype(F32)
        for dr, dq in ((0, 0),) + STEPS:
            n = place((-dr) % RING, dq)
            shift = ((n - line_index(dr, dq)) * CAP) % 128
            moved = jnp.where(lane // CAP == n, pltpu.roll(tags, shift, 1), 0.0)
            (tag_line if n == 0 else tag_out)[n] = moved

    def make_gates():
        row = lax.broadcasted_iota(jnp.int32, (HALF, 128), 0)
        lane = lax.broadcasted_iota(jnp.int32, (HALF, 128), 1)
        for n, (half, dy, dz) in enumerate(ORDER):
            tags = tag_all[dy * RING + dz][0:1, :]
            lanes = jnp.zeros_like(tags)
            for task in range(4):
                lanes = jnp.where(tags == float(task), gate_smem[task, blk], lanes)
            picked = jnp.where(lane == row + half * HALF, jnp.broadcast_to(lanes, (HALF, 128)), 0.0)
            gates[n] = jnp.broadcast_to(jnp.sum(picked, axis=1, keepdims=True), (HALF, 128))

    def forward(k):
        four = pl.ds(k * CHUNK, CHUNK)
        span = pl.ds(pl.multiple_of((k % 2) * ROWS, ROWS), ROWS)
        gate = gates[four].reshape(ROWS, 128)
        for n in range(rows.shape[3] // 128):
            cols = pl.ds(n * 128, 128)
            cot = rows[four, 1, :, cols].reshape(ROWS, 128).astype(F32)
            sc[span, cols] = (gate * cot).astype(BF16)

        def body(n, _):
            cols = pl.ds(pl.multiple_of(n * NT, NT), NT)
            pre = jnp.dot(rows[four, 0].reshape(ROWS, rows.shape[3]), w1[:, cols], preferred_element_type=F32)
            back = jnp.dot(sc[span, :], w2t[:, cols], preferred_element_type=F32)
            sig = 0.5 * jnp.tanh(0.5 * pre) + 0.5
            value = pre * sig
            act[span, cols] = value.astype(BF16)
            pg[span, cols] = (back * (sig + value * (1.0 - sig))).astype(BF16)
            return 0

        lax.fori_loop(0, w1.shape[1] // NT, body, 0)

    def row_grads(k, r):
        span = pl.ds(pl.multiple_of((k % 2) * ROWS, ROWS), ROWS)

        def body(n, _):
            cols = pl.ds(pl.multiple_of(n * NT, NT), NT)
            part = jnp.dot(pg[span, :], w1t[:, cols], preferred_element_type=F32)
            rgb[pl.ds(r * CHUNK, CHUNK), :, cols] = part.reshape(CHUNK, HALF, NT)
            return 0

        lax.fori_loop(0, w1t.shape[1] // NT, body, 0)

    def turn(k):
        eight = pl.ds((k - 1) * CHUNK, 2 * CHUNK)
        width = xt.shape[0]
        for n in range(width // 256):
            cols = pl.ds(pl.multiple_of(yhi * width + n * 256, 256), 256)
            xt[pl.ds(n * 256, 256), :] = rows[eight, 0, :, cols].reshape(PAIR, 256).T
        width = actt.shape[0]
        for n in range(width // 256):
            cols = pl.ds(pl.multiple_of(yhi * width + n * 256, 256), 256)
            actt[pl.ds(n * 256, 256), :] = act[:, cols].T

    def grads():
        def body_in(n, _):
            cols = pl.ds(pl.multiple_of(n * NT, NT), NT)
            gin[:, cols] += jnp.dot(xt[...], pg[:, cols], preferred_element_type=F32)
            return 0

        def body_out(n, _):
            cols = pl.ds(pl.multiple_of(n * 256, 256), 256)
            gout[:, cols] += jnp.dot(actt[...], sc[:, cols], preferred_element_type=F32)
            return 0

        lax.fori_loop(0, gin.shape[1] // NT, body_in, 0)
        lax.fori_loop(0, gout.shape[1] // 256, body_out, 0)

    def last_grads():
        def body_in(n, _):
            cols = pl.ds(pl.multiple_of(n * NT, NT), NT)
            gin[:, cols] = (gin[:, cols] + jnp.dot(xt[...], pg[:, cols], preferred_element_type=F32)) * grad_scale
            return 0

        def body_out(n, _):
            cols = pl.ds(pl.multiple_of(n * 256, 256), 256)
            gout[:, cols] = (gout[:, cols] + jnp.dot(actt[...], sc[:, cols], preferred_element_type=F32)) * grad_scale
            return 0

        lax.fori_loop(0, gin.shape[1] // NT, body_in, 0)
        lax.fori_loop(0, gout.shape[1] // 256, body_out, 0)

    for copy in line_copies(0, 0):
        copy.start()
    for n in range(2):
        weight_copy(n).start()

    barrier = pltpu.get_barrier_semaphore()
    around = [(dy, dz) for dy in range(RING) for dz in range(RING) if dy or dz]
    for step in STEPS:
        pl.semaphore_signal(barrier, inc=1, device_id=on_line(*step), device_id_type=MESH)
    for step in around:
        pl.semaphore_signal(barrier, inc=1, device_id=on_plane(*step), device_id_type=MESH)
    make_tags()
    pl.semaphore_wait(barrier, LINE - 1 + RING * RING - 1)

    for step in STEPS:
        tag_line_copy(*step).start()
    for step in STEPS:
        for copy in line_copies(*step):
            copy.start()

    send_piece(0)
    send_piece(1)
    for n in range(1, LINE):
        arrive(tag_line.at[n], tagp_sem.at[n])
    tags = tag_line[0]
    for n in range(1, LINE):
        tags = tags + tag_line[n]
    tag_all[0] = tags
    for step in around:
        tag_copy(*step).start()
    for n in range(2, LINE):
        send_piece(n)

    gin[...] = jnp.zeros_like(gin)
    gout[...] = jnp.zeros_like(gout)
    for n in range(2):
        weight_copy(n).wait()
    transpose_weights()
    others = tag_all.at[pl.ds(1, RING * RING - 1)]
    arrive(others, tag_sem)
    make_gates()

    def step(k, _):
        @pl.when(k == 0)
        def _():
            wait_slots((A, 0, 1), (A, 0, 3), (A, 1, 0), (A, 3, 0))
            send_hops("z4", "y3")

        @pl.when(k == 1)
        def _():
            wait_slots((B, 0, 1), (B, 0, 3), (B, 3, 0), (B, 1, 0))
            send_hops("y4", "z3", "y5", "z5")

        @pl.when(k == 2)
        def _():
            wait_slots((A, 1, 1), (A, 1, 3), (B, 0, 2))
            send_hops("y6", "y7", "z6", "z7")
            wait_slots((B, 3, 1), (B, 1, 1), (A, 2, 0))
            send_hops("z8")

        @pl.when(k == 3)
        def _():
            wait_slots((A, 0, 2), (A, 1, 2), (B, 3, 3), (B, 3, 2))

        @pl.when(k == 6)
        def _():
            for half, dz in ((A, 1), (B, 3)):
                arrive(zq.at[half], zq_sem.at[half])
                zs[half, 1 if dz == 1 else 2] = (total(half, dz) + zq[half].astype(F32)).astype(BF16)
            z_copy(A, 1).start()
            z_copy(B, 3).start()
            wait_slots((B, 2, 0), (B, 2, 1))

        @pl.when(k == 7)
        def _():
            wait_slots((A, 3, 2), (A, 2, 2), (B, 2, 3), (B, 2, 2))

        forward(k)

        @pl.when(k < OWED)
        def _():
            row_grads(k, k)

        @pl.when(k == 2)
        def _():
            y_send((A, 1), (A, 3), (B, 1))

        @pl.when(k == 3)
        def _():
            y_send((A, 2), (B, 2), (B, 3), (A, 0), (B, 0))
            wait_slots((B, 1, 3), (B, 1, 2))
            send_hops("y8", "y9", "y10")

        @pl.when(k == 4)
        def _():
            for half, dz in ((A, 3), (B, 1)):
                zs[half, 1 if dz == 1 else 2] = total(half, dz).astype(BF16)
            z_copy(A, 3).start()
            z_copy(B, 1).start()
            wait_slots((A, 3, 1), (A, 3, 3))
            send_hops("z9")

        @pl.when(k == 5)
        def _():
            for half in (A, B):
                zs[half, 0] = total(half, 2).astype(BF16)
            for half in (A, B):
                relay_copy(half).start()
            wait_slots((A, 2, 1), (A, 2, 3))
            send_hops("z10")

        @pl.when(k == 6)
        def _():
            for half in (A, B):
                value = total(half, 0)
                for n in range(2):
                    arrive(zr.at[half, n], zr_sem.at[half, n])
                    value = value + zr[half, n].astype(F32)
                fs[pl.ds(half * HALF, HALF), :] = value.astype(BF16)
            for dr, dq in STEPS:
                home_copy(dr, dq).start()
            home[cap_rows(me), :] = fs[pl.ds(0, CAP), :]

        @pl.when(k % 2 == 1)
        def _():
            turn(k)

            @pl.when(k < 7)
            def _():
                grads()

            @pl.when(k == 7)
            def _():
                last_grads()

        return 0

    lax.fori_loop(0, len(ORDER) // CHUNK, step, 0)

    for dr, dq in STEPS:
        arrive(home.at[cap_rows(line_index(dr, dq))], home_sem.at[place(dr, dq)])
    home_ref[...] = home[...]

    for dr, dq in STEPS:
        tag_line_copy(dr, dq).wait_send()
        for copy in line_copies(dr, dq):
            copy.wait_send()
        home_copy(dr, dq).wait_send()
    arrive(others, tag_send)
    for name in HOPS:
        for n in range(2):
            hop_copy(name, n).wait_send()
    for half in (A, B):
        for dz in range(RING):
            y_copy(half, dz).wait_send()
        relay_copy(half).wait_send()
        for dz in (1, 3):
            z_copy(half, dz).wait_send()


def write_out(home_ref, gin_ref, gout_ref, home_hbm, gin_hbm, gout_hbm, home32, sem):
    copies = [pltpu.make_async_copy(gin_ref, gin_hbm, sem.at[0]), pltpu.make_async_copy(gout_ref, gout_hbm, sem.at[1])]
    for copy in copies:
        copy.start()
    home32[...] = home_ref[...].astype(F32)
    copies.append(pltpu.make_async_copy(home32, home_hbm, sem.at[2]))
    copies[2].start()
    for copy in copies:
        copy.wait()


def on_device(inputs, cotangent, task_ids, group_counts, task_gate, w_in, w_out):
    rows, width = inputs.shape
    hidden = w_in.shape[2]
    any_space = pl.BlockSpec(memory_space=pl.ANY)
    hbm = pl.BlockSpec(memory_space=pltpu.HBM)
    smem = pl.BlockSpec(memory_space=pltpu.SMEM)
    vmem = pl.BlockSpec(memory_space=pltpu.VMEM)
    dma = pltpu.SemaphoreType.DMA
    home, gin, gout = pl.pallas_call(
        kernel,
        out_shape=(
            jax.ShapeDtypeStruct((rows, width), BF16),
            jax.ShapeDtypeStruct((width // 2, hidden), F32),
            jax.ShapeDtypeStruct((hidden // 2, width), F32),
        ),
        in_specs=[hbm, hbm, vmem, smem, smem, hbm, hbm],
        out_specs=(vmem,) * 3,
        scratch_shapes=[
            pltpu.VMEM((len(ORDER), 2, HALF, width), BF16),
            pltpu.VMEM((width, hidden), BF16),
            pltpu.VMEM((hidden, width), BF16),
            pltpu.VMEM((hidden, width), BF16),
            pltpu.VMEM((width, hidden), BF16),
            pltpu.VMEM((PAIR, width), BF16),
            pltpu.VMEM((PAIR, hidden), BF16),
            pltpu.VMEM((PAIR, hidden), BF16),
            pltpu.VMEM((width // 2, PAIR), BF16),
            pltpu.VMEM((hidden // 2, PAIR), BF16),
            pltpu.VMEM((len(ORDER), HALF, 128), F32),
            pltpu.VMEM((LINE, 8, LINE * CAP), F32),
            pltpu.VMEM((LINE, 8, LINE * CAP), F32),
            pltpu.VMEM((RING * RING, 8, LINE * CAP), F32),
            pltpu.VMEM((OWED * CHUNK, HALF, width), F32),
            pltpu.VMEM((2, RING, HALF, width), BF16),
            pltpu.VMEM((2, RING, HALF, width), BF16),
            pltpu.VMEM((2, 3, HALF, width), BF16),
            pltpu.VMEM((2, HALF, width), BF16),
            pltpu.VMEM((2, 2, HALF, width), BF16),
            pltpu.VMEM((2 * HALF, width), BF16),
            pltpu.VMEM((2 * HALF, width), BF16),
            dma((2,)),
            dma((LINE,)),
            dma((LINE,)),
            dma((LINE,)),
            dma((LINE, 2)),
            dma(()),
            dma(()),
            dma((len(ORDER),)),
            dma((2 * len(HOPS),)),
            dma((2, RING)),
            dma((2, RING)),
            dma((2,)),
            dma((2,)),
            dma((2, 2)),
            dma((2, 2)),
            dma((LINE,)),
            dma((LINE,)),
        ],
        compiler_params=pltpu.CompilerParams(
            collective_id=0, has_side_effects=True, vmem_limit_bytes=VMEM_LIMIT
        ),
    )(inputs, cotangent, task_ids.reshape(1, rows), group_counts, task_gate, w_in[0], w_out[0])
    home, gin, gout = pl.pallas_call(
        write_out,
        out_shape=(
            jax.ShapeDtypeStruct((rows, width), F32),
            jax.ShapeDtypeStruct((width // 2, hidden), F32),
            jax.ShapeDtypeStruct((hidden // 2, width), F32),
        ),
        in_specs=[vmem, any_space, any_space],
        out_specs=(any_space,) * 3,
        scratch_shapes=[pltpu.VMEM((rows, width), F32), dma((3,))],
        compiler_params=pltpu.CompilerParams(vmem_limit_bytes=4 * 1024 * 1024),
    )(home, gin, gout)
    return home, gin[None], gout[None]


def solution(mesh):
    in_specs = (
        P(("blk", "dp"), None),
        P(("blk", "dp"), None),
        P(("blk", "dp")),
        P(("blk", "dp"), None),
        P(),
        P("blk", None, None),
        P("blk", None, None),
    )
    out_specs = (P(("blk", "dp"), None), P("blk", "dp", None), P("blk", "dp", None))
    return jax.shard_map(on_device, mesh=mesh, in_specs=in_specs, out_specs=out_specs, check_vma=False)
```

```python
import jax
import jax.numpy as jnp
from jax import lax
from jax.experimental import pallas as pl
from jax.experimental.pallas import tpu as pltpu
from jax.sharding import PartitionSpec as P

MESH = pl.DeviceIdType.MESH
F32, BF16 = jnp.float32, jnp.bfloat16
grad_scale = 0.0625

RING = 4
LINE = 8
CAP = 16
HALF = LINE * CAP // 2
PART = HALF // 2
CHUNK = 4
ROWS = CHUNK * HALF
PAIR = 2 * ROWS
NT = 1024
RT = 512
GT_IN = 1024
GT_OUT = 512
VMEM_LIMIT = 46 * 1024 * 1024

A, B = 0, 1
ORDER = (
    (A, 0, 0), (B, 0, 0), (A, 0, 1), (A, 0, 3),
    (A, 1, 0), (B, 0, 1), (B, 0, 3), (B, 3, 0),
    (A, 1, 1), (A, 1, 3), (B, 3, 1), (B, 0, 2),
    (A, 0, 2), (A, 1, 2), (B, 3, 3), (B, 3, 2),
    (A, 3, 0), (B, 1, 0), (B, 1, 1), (B, 1, 3),
    (A, 2, 0), (B, 1, 2), (A, 3, 1), (A, 3, 3),
    (A, 2, 1), (A, 2, 3), (B, 2, 0), (B, 2, 1),
    (A, 3, 2), (A, 2, 2), (B, 2, 3), (B, 2, 2),
)
SLOT = {key: n for n, key in enumerate(ORDER)}
OWED = 4


def place(r, q):
    return {0: 0, 1: 2, 3: 4, 2: 6}[r] + q


STEPS = ((0, 1), (1, 0), (3, 0), (1, 1), (3, 1), (2, 0), (2, 1))


def dot_t(left, right):
    return lax.dot_general(left, right, (((1,), (1,)), ((), ())), preferred_element_type=F32)


def hops():
    table = {}

    def add(name, axis, half, dy, dz, split):
        for sign in (1, -1):
            if split:
                if axis == "y":
                    dy_s, dz_s = (-sign * dy) % RING, dz
                else:
                    dy_s, dz_s = dy, (-sign * dz) % RING
                part = 0 if sign == 1 else 1
            else:
                dy_s, dz_s, part = dy, dz, None
            there = (half, (dy_s - sign) % RING, dz_s) if axis == "y" else (half, dy_s, (dz_s - sign) % RING)
            table.setdefault(name, []).append((axis, sign, (half, dy_s, dz_s), part, there))

    add("y1", "y", A, 0, 0, False)
    add("y2", "y", B, 0, 0, False)
    add("y3", "y", A, 1, 0, True)
    add("y4", "y", B, 0, 1, False)
    add("y5", "y", B, 0, 3, False)
    add("y6", "y", B, 0, 2, False)
    add("y7", "y", B, 1, 0, True)
    add("y8", "y", B, 1, 1, True)
    add("y9", "y", B, 1, 3, True)
    add("y10", "y", B, 1, 2, True)
    add("z1", "z", B, 0, 0, False)
    add("z2", "z", A, 0, 0, False)
    add("z3", "z", B, 0, 1, True)
    add("z4", "z", A, 1, 0, False)
    add("z7", "z", A, 3, 0, False)
    add("z5", "z", A, 0, 1, True)
    add("z6", "z", A, 1, 1, True)
    add("z8", "z", A, 2, 0, False)
    add("z9", "z", A, 3, 1, True)
    add("z10", "z", A, 2, 1, True)
    return table


HOPS = hops()
HOP_SEM = {name: 2 * n for n, name in enumerate(HOPS)}


def kernel(
    x_hbm, cot_hbm, ids_hbm, count_smem, gate_smem, w1_hbm, w2_hbm,
    home_ref, gin, gout,
    rows, w1, w2, sc, act, pg, xt, actt, gates, tag_out, tag_line, tag_all,
    rgb, ys, ry, zs, zq, zr, fs, home, ids_ref,
    local_sem, tagp_sem, tagp_send, line_sem, line_send, tag_sem, tag_send, slot_sem, hop_send,
    ry_sem, ry_send, zq_sem, zq_send, zr_sem, zr_send, home_sem, home_send,
):
    blk, yhi = lax.axis_index("blk"), lax.axis_index("dp")
    c = blk % 2
    x = (blk // 2) % RING
    y = yhi * 2 + (blk // LINE) % 2
    z = blk // (2 * LINE)
    me = x * 2 + c

    def line_index(dr, dq):
        return ((x + dr) % RING) * 2 + (c + dq) % 2

    def on_line(dr, dq):
        return ((z * 2 + y % 2) * LINE + line_index(dr, dq), yhi)

    def on_plane(dy, dz):
        ty, tz = (y + dy) % RING, (z + dz) % RING
        return ((tz * 2 + ty % 2) * LINE + me, ty // 2)

    def remote(src, dst, recv, send, device):
        return pltpu.make_async_remote_copy(
            src_ref=src, dst_ref=dst, send_sem=send, recv_sem=recv, device_id=device, device_id_type=MESH
        )

    def arrive(ref, sem):
        pltpu.make_async_copy(ref, ref, sem).wait()

    def weight_copy(n):
        return pltpu.make_async_copy((w1_hbm, w2_hbm)[n], (w1, w2)[n], local_sem.at[n])

    def cap_rows(j):
        return pl.ds(pl.multiple_of(j * CAP, CAP), CAP)

    def piece(n):
        return n // CHUNK, pl.ds((n % CHUNK) * CAP, CAP)

    def line_copies(dr, dq):
        there = place((-dr) % RING, dq)
        here = cap_rows(line_index(dr, dq))
        slot, span = piece(there)
        for kind, src in ((0, x_hbm), (1, cot_hbm)):
            if (dr, dq) == (0, 0):
                yield pltpu.make_async_copy(src.at[here], rows.at[slot, kind, span], line_sem.at[there])
            else:
                send = line_send.at[there, kind]
                yield remote(src.at[here], rows.at[slot, kind, span], line_sem.at[there], send, on_line(dr, dq))

    def tag_line_copy(dr, dq):
        there = place((-dr) % RING, dq)
        return remote(tag_out.at[there], tag_line.at[there], tagp_sem.at[there], tagp_send.at[there], on_line(dr, dq))

    def tag_copy(dy, dz):
        there = ((-dy) % RING) * RING + (-dz) % RING
        return remote(tag_all.at[0], tag_all.at[there], tag_sem, tag_send, on_plane(dy, dz))

    def hop_copy(name, n, span=None):
        axis, sign, here, part, there = HOPS[name][n]
        if part is not None:
            span = pl.ds(part * PART, PART)
        src, dst = rows.at[SLOT[here]], rows.at[SLOT[there]]
        if span is not None:
            src, dst = rows.at[SLOT[here], :, span], rows.at[SLOT[there], :, span]
        device = on_plane(sign, 0) if axis == "y" else on_plane(0, sign)
        return remote(src, dst, slot_sem.at[SLOT[there]], hop_send.at[HOP_SEM[name] + n], device)

    def send_hops(*names):
        for name in names:
            for n in range(2):
                hop_copy(name, n).start()

    def send_piece(n):
        half, span = piece(n)
        arrive(rows.at[half, :, span], line_sem.at[n])
        for name in (("y1", "z2"), ("y2", "z1"))[half]:
            for m in range(2):
                hop_copy(name, m, span).start()

    def wait_slots(*keys):
        for key in keys:
            arrive(rows.at[SLOT[key]], slot_sem.at[SLOT[key]])

    def y_copy(half, dz):
        device = on_plane(1 if half == A else 3, 0)
        return remote(ys.at[half, dz], ry.at[half, dz], ry_sem.at[half, dz], ry_send.at[half, dz], device)

    def y_send(*keys):
        for half, dz in keys:
            ys[half, dz] = rgb[SLOT[(half, 1 if half == A else 3, dz)]].astype(BF16)
        for half, dz in keys:
            y_copy(half, dz).start()

    def relay_copy(half):
        return remote(zs.at[half, 0], zq.at[half], zq_sem.at[half], zq_send.at[half], on_plane(0, 1 if half == A else 3))

    def z_copy(half, dz):
        n = 0 if dz == 1 else 1
        return remote(zs.at[half, 1 + n], zr.at[half, n], zr_sem.at[half, n], zr_send.at[half, n], on_plane(0, dz))

    def home_copy(dr, dq):
        n = place(dr, dq)
        there = place((-dr) % RING, dq)
        src = fs.at[pl.ds(n * CAP, CAP)]
        return remote(src, home.at[cap_rows(me)], home_sem.at[there], home_send.at[n], on_line(dr, dq))

    def total(half, dz):
        arrive(ry.at[half, dz], ry_sem.at[half, dz])
        return rgb[SLOT[(half, 0, dz)]] + ry[half, dz].astype(F32)

    def make_tags():
        lane = lax.broadcasted_iota(jnp.int32, (8, 128), 1)
        count = jnp.zeros_like(lane)
        for group in range(LINE):
            count = jnp.where(lane // CAP == group, count_smem[0, group], count)
        tags = jnp.where(lane % CAP < count, jnp.broadcast_to(ids_ref[...], (8, 128)), 4).astype(F32)
        for dr, dq in ((0, 0),) + STEPS:
            n = place((-dr) % RING, dq)
            shift = ((n - line_index(dr, dq)) * CAP) % 128
            moved = jnp.where(lane // CAP == n, pltpu.roll(tags, shift, 1), 0.0)
            (tag_line if n == 0 else tag_out)[n] = moved

    def make_gates():
        row = lax.broadcasted_iota(jnp.int32, (HALF, 128), 0)
        lane = lax.broadcasted_iota(jnp.int32, (HALF, 128), 1)
        for n, (half, dy, dz) in enumerate(ORDER):
            tags = tag_all[dy * RING + dz][0:1, :]
            lanes = jnp.zeros_like(tags)
            for task in range(4):
                lanes = jnp.where(tags == float(task), gate_smem[task, blk], lanes)
            picked = jnp.where(lane == row + half * HALF, jnp.broadcast_to(lanes, (HALF, 128)), 0.0)
            gates[n] = jnp.broadcast_to(jnp.sum(picked, axis=1, keepdims=True), (HALF, 128))

    def forward(k):
        four = pl.ds(k * CHUNK, CHUNK)
        span = pl.ds(pl.multiple_of((k % 2) * ROWS, ROWS), ROWS)
        gate = gates[four].reshape(ROWS, 128)
        for n in range(rows.shape[3] // 128):
            cols = pl.ds(n * 128, 128)
            cot = rows[four, 1, :, cols].reshape(ROWS, 128).astype(F32)
            sc[span, cols] = (gate * cot).astype(BF16)

        def body(n, _):
            cols = pl.ds(pl.multiple_of(n * NT, NT), NT)
            pre = jnp.dot(rows[four, 0].reshape(ROWS, rows.shape[3]), w1[:, cols], preferred_element_type=F32)
            back = dot_t(sc[span, :], w2[cols, :])
            sig = 0.5 * jnp.tanh(0.5 * pre) + 0.5
            value = pre * sig
            act[span, cols] = value.astype(BF16)
            pg[span, cols] = (back * (sig + value * (1.0 - sig))).astype(BF16)
            return 0

        lax.fori_loop(0, w1.shape[1] // NT, body, 0)

    def row_grads(k, r):
        span = pl.ds(pl.multiple_of((k % 2) * ROWS, ROWS), ROWS)

        def body(n, _):
            cols = pl.ds(pl.multiple_of(n * RT, RT), RT)
            part = dot_t(pg[span, :], w1[cols, :])
            rgb[pl.ds(r * CHUNK, CHUNK), :, cols] = part.reshape(CHUNK, HALF, RT)
            return 0

        lax.fori_loop(0, w1.shape[0] // RT, body, 0)

    def turn(slots, first, count):
        width = xt.shape[0]
        for n in range(width // 256):
            cols = pl.ds(pl.multiple_of(yhi * width + n * 256, 256), 256)
            xt[pl.ds(n * 256, 256), pl.ds(0, count)] = rows[slots, 0, :, cols].reshape(count, 256).T
        width = actt.shape[0]
        for n in range(width // 256):
            cols = pl.ds(pl.multiple_of(yhi * width + n * 256, 256), 256)
            actt[pl.ds(n * 256, 256), pl.ds(0, count)] = act[pl.ds(first, count), cols].T

    def grads(first, count, last=False):
        here, span = pl.ds(0, count), pl.ds(first, count)

        def add(acc, cols, value):
            value = acc[:, cols] + value
            acc[:, cols] = value * grad_scale if last else value

        def body_in(n, _):
            cols = pl.ds(pl.multiple_of(n * GT_IN, GT_IN), GT_IN)
            add(gin, cols, jnp.dot(xt[:, here], pg[span, cols], preferred_element_type=F32))
            return 0

        def body_out(n, _):
            cols = pl.ds(pl.multiple_of(n * GT_OUT, GT_OUT), GT_OUT)
            add(gout, cols, jnp.dot(actt[:, here], sc[span, cols], preferred_element_type=F32))
            return 0

        lax.fori_loop(0, gin.shape[1] // GT_IN, body_in, 0)
        lax.fori_loop(0, gout.shape[1] // GT_OUT, body_out, 0)

    ids_copy = pltpu.make_async_copy(ids_hbm, ids_ref, local_sem.at[2])
    ids_copy.start()
    for copy in line_copies(0, 0):
        copy.start()
    for n in range(2):
        weight_copy(n).start()

    barrier = pltpu.get_barrier_semaphore()
    around = [(dy, dz) for dy in range(RING) for dz in range(RING) if dy or dz]
    for step in STEPS:
        pl.semaphore_signal(barrier, inc=1, device_id=on_line(*step), device_id_type=MESH)
    for step in around:
        pl.semaphore_signal(barrier, inc=1, device_id=on_plane(*step), device_id_type=MESH)
    ids_copy.wait()
    make_tags()
    pl.semaphore_wait(barrier, LINE - 1 + RING * RING - 1)

    for step in STEPS:
        tag_line_copy(*step).start()
    for step in STEPS:
        for copy in line_copies(*step):
            copy.start()

    send_piece(0)
    send_piece(1)
    for n in range(1, LINE):
        arrive(tag_line.at[n], tagp_sem.at[n])
    tags = tag_line[0]
    for n in range(1, LINE):
        tags = tags + tag_line[n]
    tag_all[0] = tags
    for step in around:
        tag_copy(*step).start()
    for n in range(2, LINE):
        send_piece(n)

    gin[...] = jnp.zeros_like(gin)
    gout[...] = jnp.zeros_like(gout)
    for n in range(2):
        weight_copy(n).wait()
    others = tag_all.at[pl.ds(1, RING * RING - 1)]
    arrive(others, tag_sem)
    make_gates()

    def step(k, _):
        @pl.when(k == 0)
        def _():
            wait_slots((A, 0, 1), (A, 0, 3), (A, 1, 0), (A, 3, 0))
            send_hops("z4", "y3")

        @pl.when(k == 1)
        def _():
            wait_slots((B, 0, 1), (B, 0, 3), (B, 3, 0), (B, 1, 0))
            send_hops("y4", "z3", "y5", "z5")

        @pl.when(k == 2)
        def _():
            wait_slots((A, 1, 1), (A, 1, 3), (B, 0, 2))
            send_hops("y6", "z6", "z7")
            wait_slots((B, 3, 1), (B, 1, 1), (A, 2, 0))
            send_hops("z8")

        @pl.when(k == 3)
        def _():
            wait_slots((A, 0, 2), (A, 1, 2), (B, 3, 3), (B, 3, 2))

        @pl.when(k == 6)
        def _():
            for half, dz in ((A, 1), (B, 3)):
                arrive(zq.at[half], zq_sem.at[half])
                zs[half, 1 if dz == 1 else 2] = (total(half, dz) + zq[half].astype(F32)).astype(BF16)
            z_copy(A, 1).start()
            z_copy(B, 3).start()
            wait_slots((B, 2, 0), (B, 2, 1))

        @pl.when(k == 7)
        def _():
            wait_slots((A, 3, 2), (A, 2, 2), (B, 2, 3), (B, 2, 2))

        forward(k)

        @pl.when(k < OWED)
        def _():
            row_grads(k, k)

        @pl.when(k == 2)
        def _():
            y_send((A, 1), (B, 1))
            send_hops("y7")

        @pl.when(k == 3)
        def _():
            y_send((A, 2), (B, 2))
            y_send((A, 3), (B, 3), (A, 0), (B, 0))
            wait_slots((B, 1, 3), (B, 1, 2))
            send_hops("y8", "y9", "y10")
            wait_slots((A, 3, 1), (A, 3, 3))
            send_hops("z9")

        @pl.when(k == 4)
        def _():
            wait_slots((A, 2, 1), (A, 2, 3))
            send_hops("z10")

        @pl.when(k == 5)
        def _():
            for half in (A, B):
                zs[half, 0] = total(half, 2).astype(BF16)
            for half in (A, B):
                relay_copy(half).start()
            for half, dz in ((A, 3), (B, 1)):
                zs[half, 1 if dz == 1 else 2] = total(half, dz).astype(BF16)
            z_copy(A, 3).start()
            z_copy(B, 1).start()

        @pl.when((k % 2 == 1) & (k < 6))
        def _():
            turn(pl.ds((k - 1) * CHUNK, 2 * CHUNK), 0, PAIR)
            grads(0, PAIR)

        @pl.when(k == 6)
        def _():
            turn(pl.ds(6 * CHUNK, CHUNK), 0, ROWS)
            grads(0, ROWS)

        @pl.when(k == 7)
        def _():
            for half in (A, B):
                value = total(half, 0)
                for n in range(2):
                    arrive(zr.at[half, n], zr_sem.at[half, n])
                    value = value + zr[half, n].astype(F32)
                fs[pl.ds(half * HALF, HALF), :] = value.astype(BF16)
            for dr, dq in STEPS:
                home_copy(dr, dq).start()
            home[cap_rows(me), :] = fs[pl.ds(0, CAP), :]
            turn(pl.ds(7 * CHUNK, CHUNK), ROWS, ROWS)
            grads(ROWS, ROWS, last=True)

        return 0

    lax.fori_loop(0, len(ORDER) // CHUNK, step, 0)

    for dr, dq in STEPS:
        arrive(home.at[cap_rows(line_index(dr, dq))], home_sem.at[place(dr, dq)])
    home_ref[...] = home[...]

    for dr, dq in STEPS:
        tag_line_copy(dr, dq).wait_send()
        for copy in line_copies(dr, dq):
            copy.wait_send()
        home_copy(dr, dq).wait_send()
    arrive(others, tag_send)
    for name in HOPS:
        for n in range(2):
            hop_copy(name, n).wait_send()
    for half in (A, B):
        for dz in range(RING):
            y_copy(half, dz).wait_send()
        relay_copy(half).wait_send()
        for dz in (1, 3):
            z_copy(half, dz).wait_send()


def write_out(home_ref, gin_ref, gout_ref, home_hbm, gin_hbm, gout_hbm, home32, sem):
    copies = [pltpu.make_async_copy(gin_ref, gin_hbm, sem.at[0]), pltpu.make_async_copy(gout_ref, gout_hbm, sem.at[1])]
    for copy in copies:
        copy.start()
    home32[...] = home_ref[...].astype(F32)
    copies.append(pltpu.make_async_copy(home32, home_hbm, sem.at[2]))
    copies[2].start()
    for copy in copies:
        copy.wait()


def in_hbm(*arrays):
    return tuple(pltpu.with_memory_space_constraint(array, pltpu.HBM) for array in arrays)


def on_device(inputs, cotangent, task_ids, group_counts, task_gate, w_in, w_out):
    rows, width = inputs.shape
    hidden = w_in.shape[2]
    any_space = pl.BlockSpec(memory_space=pl.ANY)
    hbm = pl.BlockSpec(memory_space=pltpu.HBM)
    smem = pl.BlockSpec(memory_space=pltpu.SMEM)
    vmem = pl.BlockSpec(memory_space=pltpu.VMEM)
    dma = pltpu.SemaphoreType.DMA
    home, gin, gout = pl.pallas_call(
        kernel,
        out_shape=(
            pltpu.VMEM((rows, width), BF16),
            pltpu.VMEM((width // 2, hidden), F32),
            pltpu.VMEM((hidden // 2, width), F32),
        ),
        in_specs=[hbm, hbm, hbm, smem, smem, hbm, hbm],
        out_specs=(vmem,) * 3,
        scratch_shapes=[
            pltpu.VMEM((len(ORDER), 2, HALF, width), BF16),
            pltpu.VMEM((width, hidden), BF16),
            pltpu.VMEM((hidden, width), BF16),
            pltpu.VMEM((PAIR, width), BF16),
            pltpu.VMEM((PAIR, hidden), BF16),
            pltpu.VMEM((PAIR, hidden), BF16),
            pltpu.VMEM((width // 2, PAIR), BF16),
            pltpu.VMEM((hidden // 2, PAIR), BF16),
            pltpu.VMEM((len(ORDER), HALF, 128), F32),
            pltpu.VMEM((LINE, 8, LINE * CAP), F32),
            pltpu.VMEM((LINE, 8, LINE * CAP), F32),
            pltpu.VMEM((RING * RING, 8, LINE * CAP), F32),
            pltpu.VMEM((OWED * CHUNK, HALF, width), F32),
            pltpu.VMEM((2, RING, HALF, width), BF16),
            pltpu.VMEM((2, RING, HALF, width), BF16),
            pltpu.VMEM((2, 3, HALF, width), BF16),
            pltpu.VMEM((2, HALF, width), BF16),
            pltpu.VMEM((2, 2, HALF, width), BF16),
            pltpu.VMEM((2 * HALF, width), BF16),
            pltpu.VMEM((2 * HALF, width), BF16),
            pltpu.VMEM((1, 2 * HALF), jnp.int32),
            dma((3,)),
            dma((LINE,)),
            dma((LINE,)),
            dma((LINE,)),
            dma((LINE, 2)),
            dma(()),
            dma(()),
            dma((len(ORDER),)),
            dma((2 * len(HOPS),)),
            dma((2, RING)),
            dma((2, RING)),
            dma((2,)),
            dma((2,)),
            dma((2, 2)),
            dma((2, 2)),
            dma((LINE,)),
            dma((LINE,)),
        ],
        compiler_params=pltpu.CompilerParams(
            collective_id=0, has_side_effects=True, vmem_limit_bytes=VMEM_LIMIT
        ),
    )(*in_hbm(inputs, cotangent, task_ids.reshape(1, rows)), group_counts, task_gate, *in_hbm(w_in[0], w_out[0]))
    home, gin, gout = pl.pallas_call(
        write_out,
        out_shape=(
            jax.ShapeDtypeStruct((rows, width), F32),
            jax.ShapeDtypeStruct((width // 2, hidden), F32),
            jax.ShapeDtypeStruct((hidden // 2, width), F32),
        ),
        in_specs=[vmem, any_space, any_space],
        out_specs=(any_space,) * 3,
        scratch_shapes=[pltpu.VMEM((rows, width), F32), dma((3,))],
        compiler_params=pltpu.CompilerParams(vmem_limit_bytes=4 * 1024 * 1024),
    )(home, gin, gout)
    return home, gin[None], gout[None]


def solution(mesh):
    in_specs = (
        P(("blk", "dp"), None),
        P(("blk", "dp"), None),
        P(("blk", "dp")),
        P(("blk", "dp"), None),
        P(),
        P("blk", None, None),
        P("blk", None, None),
    )
    out_specs = (P(("blk", "dp"), None), P("blk", "dp", None), P("blk", "dp", None))
    return jax.shard_map(on_device, mesh=mesh, in_specs=in_specs, out_specs=out_specs, check_vma=False)
```

```python
import jax
import jax.numpy as jnp
from jax import lax
from jax.experimental import pallas as pl
from jax.experimental.pallas import tpu as pltpu
from jax.sharding import PartitionSpec as P

MESH = pl.DeviceIdType.MESH
F32, BF16 = jnp.float32, jnp.bfloat16
grad_scale = 0.0625

RING = 4
LINE = 8
CAP = 16
HALF = LINE * CAP // 2
PART = HALF // 2
CHUNK = 4
ROWS = CHUNK * HALF
PAIR = 2 * ROWS
NT = 1024
RT = 512
GT_IN = 1024
GT_OUT = 512
VMEM_LIMIT = 46 * 1024 * 1024

A, B = 0, 1
ORDER = (
    (A, 0, 0), (B, 0, 0), (A, 0, 1), (A, 0, 3),
    (A, 1, 0), (B, 0, 1), (B, 0, 3), (B, 3, 0),
    (A, 1, 1), (A, 1, 3), (B, 3, 1), (B, 0, 2),
    (A, 3, 0), (B, 1, 0), (B, 1, 1), (B, 1, 3),
    (A, 0, 2), (A, 1, 2), (B, 3, 3), (B, 3, 2),
    (A, 2, 0), (B, 1, 2), (A, 3, 1), (A, 3, 3),
    (A, 2, 1), (A, 2, 3), (A, 3, 2), (B, 2, 0),
    (A, 2, 2), (B, 2, 1), (B, 2, 3), (B, 2, 2),
)
SLOT = {key: n for n, key in enumerate(ORDER)}
OWED = {0: 0, 1: 1, 2: 2, 4: 3}
OWED_SLOT = {key: OWED[n // CHUNK] * CHUNK + n % CHUNK for key, n in SLOT.items() if n // CHUNK in OWED}


def place(r, q):
    return {0: 0, 1: 2, 3: 4, 2: 6}[r] + q


STEPS = ((0, 1), (1, 0), (3, 0), (1, 1), (3, 1), (2, 0), (2, 1))


def dot_t(left, right):
    return lax.dot_general(left, right, (((1,), (1,)), ((), ())), preferred_element_type=F32)


def hops():
    table = {}

    def add(name, axis, half, dy, dz, split):
        for sign in (1, -1):
            if split:
                if axis == "y":
                    dy_s, dz_s = (-sign * dy) % RING, dz
                else:
                    dy_s, dz_s = dy, (-sign * dz) % RING
                part = 0 if sign == 1 else 1
            else:
                dy_s, dz_s, part = dy, dz, None
            there = (half, (dy_s - sign) % RING, dz_s) if axis == "y" else (half, dy_s, (dz_s - sign) % RING)
            table.setdefault(name, []).append((axis, sign, (half, dy_s, dz_s), part, there))

    add("y1", "y", A, 0, 0, False)
    add("y2", "y", B, 0, 0, False)
    add("y3", "y", A, 1, 0, True)
    add("y4", "y", B, 0, 1, False)
    add("y5", "y", B, 0, 3, False)
    add("y6", "y", B, 0, 2, False)
    add("y7", "y", B, 1, 0, True)
    add("y8", "y", B, 1, 1, True)
    add("y9", "y", B, 1, 3, True)
    add("y10", "y", B, 1, 2, True)
    add("z1", "z", B, 0, 0, False)
    add("z2", "z", A, 0, 0, False)
    add("z3", "z", B, 0, 1, True)
    add("z4", "z", A, 1, 0, False)
    add("z7", "z", A, 3, 0, False)
    add("z5", "z", A, 0, 1, True)
    add("z6", "z", A, 1, 1, True)
    add("z8", "z", A, 2, 0, False)
    add("z9", "z", A, 3, 1, True)
    add("z10", "z", A, 2, 1, True)
    return table


HOPS = hops()
HOP_SEM = {name: 2 * n for n, name in enumerate(HOPS)}


def kernel(
    x_hbm, cot_hbm, ids_hbm, count_smem, gate_smem, w1_hbm, w2_hbm,
    home_ref, gin, gout,
    rows, w1, w2, sc, act, pg, xt, actt, gates, tag_out, tag_line, tag_all,
    rgb, ys, ry, zs, zq, zr, fs, home, ids_ref,
    local_sem, tagp_sem, tagp_send, line_sem, line_send, tag_sem, tag_send, slot_sem, hop_send,
    ry_sem, ry_send, zq_sem, zq_send, zr_sem, zr_send, home_sem, home_send,
):
    blk, yhi = lax.axis_index("blk"), lax.axis_index("dp")
    c = blk % 2
    x = (blk // 2) % RING
    y = yhi * 2 + (blk // LINE) % 2
    z = blk // (2 * LINE)
    me = x * 2 + c

    def line_index(dr, dq):
        return ((x + dr) % RING) * 2 + (c + dq) % 2

    def on_line(dr, dq):
        return ((z * 2 + y % 2) * LINE + line_index(dr, dq), yhi)

    def on_plane(dy, dz):
        ty, tz = (y + dy) % RING, (z + dz) % RING
        return ((tz * 2 + ty % 2) * LINE + me, ty // 2)

    def remote(src, dst, recv, send, device):
        return pltpu.make_async_remote_copy(
            src_ref=src, dst_ref=dst, send_sem=send, recv_sem=recv, device_id=device, device_id_type=MESH
        )

    def arrive(ref, sem):
        pltpu.make_async_copy(ref, ref, sem).wait()

    def weight_copy(n):
        return pltpu.make_async_copy((w1_hbm, w2_hbm)[n], (w1, w2)[n], local_sem.at[n])

    def cap_rows(j):
        return pl.ds(pl.multiple_of(j * CAP, CAP), CAP)

    def piece(n):
        return n // CHUNK, pl.ds((n % CHUNK) * CAP, CAP)

    def line_copies(dr, dq):
        there = place((-dr) % RING, dq)
        here = cap_rows(line_index(dr, dq))
        slot, span = piece(there)
        for kind, src in ((0, x_hbm), (1, cot_hbm)):
            if (dr, dq) == (0, 0):
                yield pltpu.make_async_copy(src.at[here], rows.at[slot, kind, span], line_sem.at[there])
            else:
                send = line_send.at[there, kind]
                yield remote(src.at[here], rows.at[slot, kind, span], line_sem.at[there], send, on_line(dr, dq))

    def tag_line_copy(dr, dq):
        there = place((-dr) % RING, dq)
        return remote(tag_out.at[there], tag_line.at[there], tagp_sem.at[there], tagp_send.at[there], on_line(dr, dq))

    def tag_copy(dy, dz):
        there = ((-dy) % RING) * RING + (-dz) % RING
        return remote(tag_all.at[0], tag_all.at[there], tag_sem, tag_send, on_plane(dy, dz))

    def hop_copy(name, n, span=None):
        axis, sign, here, part, there = HOPS[name][n]
        if part is not None:
            span = pl.ds(part * PART, PART)
        src, dst = rows.at[SLOT[here]], rows.at[SLOT[there]]
        if span is not None:
            src, dst = rows.at[SLOT[here], :, span], rows.at[SLOT[there], :, span]
        device = on_plane(sign, 0) if axis == "y" else on_plane(0, sign)
        return remote(src, dst, slot_sem.at[SLOT[there]], hop_send.at[HOP_SEM[name] + n], device)

    def send_hops(*names):
        for name in names:
            for n in range(2):
                hop_copy(name, n).start()

    def send_piece(n):
        half, span = piece(n)
        arrive(rows.at[half, :, span], line_sem.at[n])
        for name in (("y1", "z2"), ("y2", "z1"))[half]:
            for m in range(2):
                hop_copy(name, m, span).start()

    def wait_slots(*keys):
        for key in keys:
            arrive(rows.at[SLOT[key]], slot_sem.at[SLOT[key]])

    def y_copy(half, dz):
        device = on_plane(1 if half == A else 3, 0)
        return remote(ys.at[half, dz], ry.at[half, dz], ry_sem.at[half, dz], ry_send.at[half, dz], device)

    def y_send(*keys):
        for half, dz in keys:
            ys[half, dz] = rgb[OWED_SLOT[(half, 1 if half == A else 3, dz)]].astype(BF16)
        for half, dz in keys:
            y_copy(half, dz).start()

    def relay_copy(half):
        return remote(zs.at[half, 0], zq.at[half], zq_sem.at[half], zq_send.at[half], on_plane(0, 1 if half == A else 3))

    def z_copy(half, dz):
        n = 0 if dz == 1 else 1
        return remote(zs.at[half, 1 + n], zr.at[half, n], zr_sem.at[half, n], zr_send.at[half, n], on_plane(0, dz))

    def home_copy(dr, dq):
        n = place(dr, dq)
        there = place((-dr) % RING, dq)
        src = fs.at[pl.ds(n * CAP, CAP)]
        return remote(src, home.at[cap_rows(me)], home_sem.at[there], home_send.at[n], on_line(dr, dq))

    def total(half, dz):
        arrive(ry.at[half, dz], ry_sem.at[half, dz])
        return rgb[OWED_SLOT[(half, 0, dz)]] + ry[half, dz].astype(F32)

    def make_tags():
        lane = lax.broadcasted_iota(jnp.int32, (8, 128), 1)
        count = jnp.zeros_like(lane)
        for group in range(LINE):
            count = jnp.where(lane // CAP == group, count_smem[0, group], count)
        tags = jnp.where(lane % CAP < count, jnp.broadcast_to(ids_ref[...], (8, 128)), 4).astype(F32)
        for dr, dq in ((0, 0),) + STEPS:
            n = place((-dr) % RING, dq)
            shift = ((n - line_index(dr, dq)) * CAP) % 128
            moved = jnp.where(lane // CAP == n, pltpu.roll(tags, shift, 1), 0.0)
            (tag_line if n == 0 else tag_out)[n] = moved

    def make_gates():
        row = lax.broadcasted_iota(jnp.int32, (HALF, 128), 0)
        lane = lax.broadcasted_iota(jnp.int32, (HALF, 128), 1)
        for n, (half, dy, dz) in enumerate(ORDER):
            tags = tag_all[dy * RING + dz][0:1, :]
            lanes = jnp.zeros_like(tags)
            for task in range(4):
                lanes = jnp.where(tags == float(task), gate_smem[task, blk], lanes)
            picked = jnp.where(lane == row + half * HALF, jnp.broadcast_to(lanes, (HALF, 128)), 0.0)
            gates[n] = jnp.broadcast_to(jnp.sum(picked, axis=1, keepdims=True), (HALF, 128))

    def forward(k):
        four = pl.ds(k * CHUNK, CHUNK)
        span = pl.ds(pl.multiple_of((k % 2) * ROWS, ROWS), ROWS)
        gate = gates[four].reshape(ROWS, 128)
        for n in range(rows.shape[3] // 128):
            cols = pl.ds(n * 128, 128)
            cot = rows[four, 1, :, cols].reshape(ROWS, 128).astype(F32)
            sc[span, cols] = (gate * cot).astype(BF16)

        def body(n, _):
            cols = pl.ds(pl.multiple_of(n * NT, NT), NT)
            pre = jnp.dot(rows[four, 0].reshape(ROWS, rows.shape[3]), w1[:, cols], preferred_element_type=F32)
            back = dot_t(sc[span, :], w2[cols, :])
            sig = 0.5 * jnp.tanh(0.5 * pre) + 0.5
            value = pre * sig
            act[span, cols] = value.astype(BF16)
            pg[span, cols] = (back * (sig + value * (1.0 - sig))).astype(BF16)
            return 0

        lax.fori_loop(0, w1.shape[1] // NT, body, 0)

    def row_grads(k, r):
        span = pl.ds(pl.multiple_of((k % 2) * ROWS, ROWS), ROWS)

        def body(n, _):
            cols = pl.ds(pl.multiple_of(n * RT, RT), RT)
            part = dot_t(pg[span, :], w1[cols, :])
            rgb[pl.ds(r * CHUNK, CHUNK), :, cols] = part.reshape(CHUNK, HALF, RT)
            return 0

        lax.fori_loop(0, w1.shape[0] // RT, body, 0)

    def turn(slots, first, count):
        width = xt.shape[0]
        for n in range(width // 256):
            cols = pl.ds(pl.multiple_of(yhi * width + n * 256, 256), 256)
            xt[pl.ds(n * 256, 256), pl.ds(0, count)] = rows[slots, 0, :, cols].reshape(count, 256).T
        width = actt.shape[0]
        for n in range(width // 256):
            cols = pl.ds(pl.multiple_of(yhi * width + n * 256, 256), 256)
            actt[pl.ds(n * 256, 256), pl.ds(0, count)] = act[pl.ds(first, count), cols].T

    def grads(first, count, last=False):
        here, span = pl.ds(0, count), pl.ds(first, count)

        def add(acc, cols, value):
            value = acc[:, cols] + value
            acc[:, cols] = value * grad_scale if last else value

        def body_in(n, _):
            cols = pl.ds(pl.multiple_of(n * GT_IN, GT_IN), GT_IN)
            add(gin, cols, jnp.dot(xt[:, here], pg[span, cols], preferred_element_type=F32))
            return 0

        def body_out(n, _):
            cols = pl.ds(pl.multiple_of(n * GT_OUT, GT_OUT), GT_OUT)
            add(gout, cols, jnp.dot(actt[:, here], sc[span, cols], preferred_element_type=F32))
            return 0

        lax.fori_loop(0, gin.shape[1] // GT_IN, body_in, 0)
        lax.fori_loop(0, gout.shape[1] // GT_OUT, body_out, 0)

    ids_copy = pltpu.make_async_copy(ids_hbm, ids_ref, local_sem.at[2])
    ids_copy.start()
    for copy in line_copies(0, 0):
        copy.start()
    for n in range(2):
        weight_copy(n).start()

    barrier = pltpu.get_barrier_semaphore()
    around = [(dy, dz) for dy in range(RING) for dz in range(RING) if dy or dz]
    for step in STEPS:
        pl.semaphore_signal(barrier, inc=1, device_id=on_line(*step), device_id_type=MESH)
    for step in around:
        pl.semaphore_signal(barrier, inc=1, device_id=on_plane(*step), device_id_type=MESH)
    ids_copy.wait()
    make_tags()
    pl.semaphore_wait(barrier, LINE - 1 + RING * RING - 1)

    for step in STEPS:
        tag_line_copy(*step).start()
    for step in STEPS:
        for copy in line_copies(*step):
            copy.start()

    send_piece(0)
    send_piece(1)
    for n in range(1, LINE):
        arrive(tag_line.at[n], tagp_sem.at[n])
    tags = tag_line[0]
    for n in range(1, LINE):
        tags = tags + tag_line[n]
    tag_all[0] = tags
    for step in around:
        tag_copy(*step).start()
    for n in range(2, LINE):
        send_piece(n)

    gin[...] = jnp.zeros_like(gin)
    gout[...] = jnp.zeros_like(gout)
    for n in range(2):
        weight_copy(n).wait()
    others = tag_all.at[pl.ds(1, RING * RING - 1)]
    arrive(others, tag_sem)
    make_gates()

    def step(k, _):
        @pl.when(k == 0)
        def _():
            wait_slots((A, 0, 1), (A, 0, 3), (A, 1, 0), (A, 3, 0))
            send_hops("z4", "y3")

        @pl.when(k == 1)
        def _():
            wait_slots((B, 0, 1), (B, 0, 3), (B, 3, 0), (B, 1, 0))
            send_hops("y4", "z3", "y5", "z5")

        @pl.when(k == 2)
        def _():
            wait_slots((A, 1, 1), (A, 1, 3), (B, 0, 2))
            send_hops("y6", "z6", "z7")
            wait_slots((B, 3, 1), (B, 1, 1), (A, 2, 0))
            send_hops("z8")

        @pl.when(k == 3)
        def _():
            wait_slots((B, 1, 3))

        @pl.when(k == 4)
        def _():
            wait_slots((A, 0, 2), (A, 1, 2), (A, 3, 1), (A, 3, 3))
            send_hops("z9")
            wait_slots((B, 3, 3), (B, 3, 2))

        @pl.when(k == 6)
        def _():
            wait_slots((A, 3, 2), (B, 2, 0))

        @pl.when(k == 7)
        def _():
            for half in (A, B):
                value = total(half, 0)
                for n in range(2):
                    arrive(zr.at[half, n], zr_sem.at[half, n])
                    value = value + zr[half, n].astype(F32)
                fs[pl.ds(half * HALF, HALF), :] = value.astype(BF16)
            for dr, dq in STEPS:
                home_copy(dr, dq).start()
            home[cap_rows(me), :] = fs[pl.ds(0, CAP), :]
            wait_slots((A, 2, 2), (B, 2, 1), (B, 2, 3), (B, 2, 2))

        forward(k)

        @pl.when((k < 3) | (k == 4))
        def _():
            row_grads(k, k - k // 4)

        @pl.when(k == 2)
        def _():
            y_send((A, 1), (B, 1))
            send_hops("y7")

        @pl.when(k == 4)
        def _():
            y_send((A, 2), (B, 2))
            y_send((A, 3), (B, 3), (A, 0), (B, 0))
            wait_slots((B, 1, 2))
            send_hops("y8", "y9", "y10")

        @pl.when(k == 5)
        def _():
            wait_slots((A, 2, 1), (A, 2, 3))
            send_hops("z10")

        @pl.when(k == 6)
        def _():
            for half, dz in ((A, 3), (B, 1)):
                zs[half, 1 if dz == 1 else 2] = total(half, dz).astype(BF16)
            z_copy(A, 3).start()
            z_copy(B, 1).start()

        @pl.when((k % 2 == 1) & (k < 6))
        def _():
            turn(pl.ds((k - 1) * CHUNK, 2 * CHUNK), 0, PAIR)
            grads(0, PAIR)

        @pl.when(k == 5)
        def _():
            for half in (A, B):
                zs[half, 0] = total(half, 2).astype(BF16)
            for half in (A, B):
                relay_copy(half).start()

        @pl.when(k == 6)
        def _():
            turn(pl.ds(6 * CHUNK, CHUNK), 0, ROWS)
            grads(0, ROWS)
            for half, dz in ((A, 1), (B, 3)):
                arrive(zq.at[half], zq_sem.at[half])
                zs[half, 1 if dz == 1 else 2] = (total(half, dz) + zq[half].astype(F32)).astype(BF16)
            z_copy(A, 1).start()
            z_copy(B, 3).start()

        @pl.when(k == 7)
        def _():
            turn(pl.ds(7 * CHUNK, CHUNK), ROWS, ROWS)
            grads(ROWS, ROWS, last=True)

        return 0

    lax.fori_loop(0, len(ORDER) // CHUNK, step, 0)

    for dr, dq in STEPS:
        arrive(home.at[cap_rows(line_index(dr, dq))], home_sem.at[place(dr, dq)])
    home_ref[...] = home[...]

    for dr, dq in STEPS:
        tag_line_copy(dr, dq).wait_send()
        for copy in line_copies(dr, dq):
            copy.wait_send()
        home_copy(dr, dq).wait_send()
    arrive(others, tag_send)
    for name in HOPS:
        for n in range(2):
            hop_copy(name, n).wait_send()
    for half in (A, B):
        for dz in range(RING):
            y_copy(half, dz).wait_send()
        relay_copy(half).wait_send()
        for dz in (1, 3):
            z_copy(half, dz).wait_send()


def write_out(home_ref, gin_ref, gout_ref, home_hbm, gin_hbm, gout_hbm, home32, sem):
    copies = [pltpu.make_async_copy(gin_ref, gin_hbm, sem.at[0]), pltpu.make_async_copy(gout_ref, gout_hbm, sem.at[1])]
    for copy in copies:
        copy.start()
    home32[...] = home_ref[...].astype(F32)
    copies.append(pltpu.make_async_copy(home32, home_hbm, sem.at[2]))
    copies[2].start()
    for copy in copies:
        copy.wait()


def in_hbm(*arrays):
    return tuple(pltpu.with_memory_space_constraint(array, pltpu.HBM) for array in arrays)


def on_device(inputs, cotangent, task_ids, group_counts, task_gate, w_in, w_out):
    rows, width = inputs.shape
    hidden = w_in.shape[2]
    any_space = pl.BlockSpec(memory_space=pl.ANY)
    hbm = pl.BlockSpec(memory_space=pltpu.HBM)
    smem = pl.BlockSpec(memory_space=pltpu.SMEM)
    vmem = pl.BlockSpec(memory_space=pltpu.VMEM)
    dma = pltpu.SemaphoreType.DMA
    home, gin, gout = pl.pallas_call(
        kernel,
        out_shape=(
            pltpu.VMEM((rows, width), BF16),
            pltpu.VMEM((width // 2, hidden), F32),
            pltpu.VMEM((hidden // 2, width), F32),
        ),
        in_specs=[hbm, hbm, hbm, smem, smem, hbm, hbm],
        out_specs=(vmem,) * 3,
        scratch_shapes=[
            pltpu.VMEM((len(ORDER), 2, HALF, width), BF16),
            pltpu.VMEM((width, hidden), BF16),
            pltpu.VMEM((hidden, width), BF16),
            pltpu.VMEM((PAIR, width), BF16),
            pltpu.VMEM((PAIR, hidden), BF16),
            pltpu.VMEM((PAIR, hidden), BF16),
            pltpu.VMEM((width // 2, PAIR), BF16),
            pltpu.VMEM((hidden // 2, PAIR), BF16),
            pltpu.VMEM((len(ORDER), HALF, 128), F32),
            pltpu.VMEM((LINE, 8, LINE * CAP), F32),
            pltpu.VMEM((LINE, 8, LINE * CAP), F32),
            pltpu.VMEM((RING * RING, 8, LINE * CAP), F32),
            pltpu.VMEM((len(OWED) * CHUNK, HALF, width), F32),
            pltpu.VMEM((2, RING, HALF, width), BF16),
            pltpu.VMEM((2, RING, HALF, width), BF16),
            pltpu.VMEM((2, 3, HALF, width), BF16),
            pltpu.VMEM((2, HALF, width), BF16),
            pltpu.VMEM((2, 2, HALF, width), BF16),
            pltpu.VMEM((2 * HALF, width), BF16),
            pltpu.VMEM((2 * HALF, width), BF16),
            pltpu.VMEM((1, 2 * HALF), jnp.int32),
            dma((3,)),
            dma((LINE,)),
            dma((LINE,)),
            dma((LINE,)),
            dma((LINE, 2)),
            dma(()),
            dma(()),
            dma((len(ORDER),)),
            dma((2 * len(HOPS),)),
            dma((2, RING)),
            dma((2, RING)),
            dma((2,)),
            dma((2,)),
            dma((2, 2)),
            dma((2, 2)),
            dma((LINE,)),
            dma((LINE,)),
        ],
        compiler_params=pltpu.CompilerParams(
            collective_id=0, has_side_effects=True, vmem_limit_bytes=VMEM_LIMIT
        ),
    )(*in_hbm(inputs, cotangent, task_ids.reshape(1, rows)), group_counts, task_gate, *in_hbm(w_in[0], w_out[0]))
    home, gin, gout = pl.pallas_call(
        write_out,
        out_shape=(
            jax.ShapeDtypeStruct((rows, width), F32),
            jax.ShapeDtypeStruct((width // 2, hidden), F32),
            jax.ShapeDtypeStruct((hidden // 2, width), F32),
        ),
        in_specs=[vmem, any_space, any_space],
        out_specs=(any_space,) * 3,
        scratch_shapes=[pltpu.VMEM((rows, width), F32), dma((3,))],
        compiler_params=pltpu.CompilerParams(vmem_limit_bytes=4 * 1024 * 1024),
    )(home, gin, gout)
    return home, gin[None], gout[None]


def solution(mesh):
    in_specs = (
        P(("blk", "dp"), None),
        P(("blk", "dp"), None),
        P(("blk", "dp")),
        P(("blk", "dp"), None),
        P(),
        P("blk", None, None),
        P("blk", None, None),
    )
    out_specs = (P(("blk", "dp"), None), P("blk", "dp", None), P("blk", "dp", None))
    return jax.shard_map(on_device, mesh=mesh, in_specs=in_specs, out_specs=out_specs, check_vma=False)
```

```python
import jax
import jax.numpy as jnp
from jax import lax
from jax.experimental import pallas as pl
from jax.experimental.pallas import tpu as pltpu
from jax.sharding import PartitionSpec as P

MESH = pl.DeviceIdType.MESH
F32, BF16 = jnp.float32, jnp.bfloat16
grad_scale = 0.0625

RING = 4
LINE = 8
CAP = 16
HALF = LINE * CAP // 2
PART = HALF // 2
CHUNK = 4
ROWS = CHUNK * HALF
PAIR = 2 * ROWS
NT = 2048
RT = 1024
GT_IN = 2048
GT_OUT = 1024
VMEM_LIMIT = 46 * 1024 * 1024

A, B = 0, 1
ORDER = (
    (A, 0, 0), (B, 0, 0), (A, 0, 1), (A, 0, 3),
    (A, 1, 0), (B, 0, 1), (B, 0, 3), (B, 3, 0),
    (A, 1, 1), (A, 1, 3), (B, 3, 1), (B, 0, 2),
    (A, 3, 0), (B, 1, 0), (B, 1, 1), (B, 1, 3),
    (A, 0, 2), (A, 1, 2), (B, 3, 3), (B, 3, 2),
    (A, 2, 0), (B, 1, 2), (A, 3, 1), (A, 3, 3),
    (A, 2, 1), (A, 2, 3), (A, 3, 2), (B, 2, 0),
    (A, 2, 2), (B, 2, 1), (B, 2, 3), (B, 2, 2),
)
SLOT = {key: n for n, key in enumerate(ORDER)}
OWED = {0: 0, 1: 1, 2: 2, 4: 3}
OWED_SLOT = {key: OWED[n // CHUNK] * CHUNK + n % CHUNK for key, n in SLOT.items() if n // CHUNK in OWED}


def place(r, q):
    return {0: 0, 1: 2, 3: 4, 2: 6}[r] + q


STEPS = ((0, 1), (1, 0), (3, 0), (1, 1), (3, 1), (2, 0), (2, 1))


def dot_t(left, right):
    return lax.dot_general(left, right, (((1,), (1,)), ((), ())), preferred_element_type=F32)


def hops():
    table = {}
    both = ((0, PART), (PART, PART))

    def add(name, axis, half, dy, dz, spans=(None, None)):
        for sign, span in zip((1, -1), spans):
            dy_s, dz_s = dy, dz
            if spans[0] is not None and spans[0] != spans[1]:
                dy_s, dz_s = ((-sign * dy) % RING, dz) if axis == "y" else (dy, (-sign * dz) % RING)
            there = (half, (dy_s - sign) % RING, dz_s) if axis == "y" else (half, dy_s, (dz_s - sign) % RING)
            table.setdefault(name, []).append((axis, sign, (half, dy_s, dz_s), span, there))

    add("y1", "y", A, 0, 0)
    add("y2", "y", B, 0, 0)
    add("y3", "y", A, 1, 0, both)
    add("y4", "y", B, 0, 1)
    add("y5", "y", B, 0, 3)
    add("y6", "y", B, 0, 2)
    add("y7", "y", B, 1, 0, both)
    add("y8", "y", B, 1, 1, both)
    add("y9", "y", B, 1, 3, both)
    add("y10", "y", B, 1, 2, both)
    add("z1", "z", B, 0, 0)
    add("z2", "z", A, 0, 0)
    add("z3", "z", B, 0, 1, both)
    add("z4", "z", A, 1, 0)
    add("z5", "z", A, 0, 1, both)
    add("z6", "z", A, 1, 1, both)
    add("z7", "z", A, 3, 0)
    add("z8", "z", A, 2, 0)
    add("z9", "z", A, 3, 1, both)
    add("z10", "z", A, 2, 1, both)
    return table


HOPS = hops()
HOP_SEM = {name: 2 * n for n, name in enumerate(HOPS)}


def kernel(
    x_hbm, cot_hbm, ids_hbm, count_smem, gate_smem, w1_hbm, w2_hbm,
    home_ref, gin, gout,
    rows, w1, w2, sc, act, pg, xt, actt, gates, tag_out, tag_line, tag_all,
    rgb, ys, ry, zs, zq, zr, fs, home, ids_ref, staged,
    local_sem, tagp_sem, tagp_send, line_sem, line_send, tag_sem, tag_send, slot_sem, hop_send,
    ry_sem, ry_send, zq_sem, zq_send, zr_sem, zr_send, home_sem, home_send,
):
    blk, yhi = lax.axis_index("blk"), lax.axis_index("dp")
    c = blk % 2
    x = (blk // 2) % RING
    y = yhi * 2 + (blk // LINE) % 2
    z = blk // (2 * LINE)
    me = x * 2 + c

    def line_index(dr, dq):
        return ((x + dr) % RING) * 2 + (c + dq) % 2

    def on_line(dr, dq):
        return ((z * 2 + y % 2) * LINE + line_index(dr, dq), yhi)

    def on_plane(dy, dz):
        ty, tz = (y + dy) % RING, (z + dz) % RING
        return ((tz * 2 + ty % 2) * LINE + me, ty // 2)

    def remote(src, dst, recv, send, device):
        return pltpu.make_async_remote_copy(
            src_ref=src, dst_ref=dst, send_sem=send, recv_sem=recv, device_id=device, device_id_type=MESH
        )

    def arrive(ref, sem):
        pltpu.make_async_copy(ref, ref, sem).wait()

    def weight_copy(n):
        return pltpu.make_async_copy((w1_hbm, w2_hbm)[n], (w1, w2)[n], local_sem.at[n])

    def cap_rows(j):
        return pl.ds(pl.multiple_of(j * CAP, CAP), CAP)

    def piece(n):
        return n // CHUNK, pl.ds((n % CHUNK) * CAP, CAP)

    def line_copies(dr, dq):
        there = place((-dr) % RING, dq)
        here = cap_rows(line_index(dr, dq))
        slot, span = piece(there)
        for kind, src in ((0, x_hbm), (1, cot_hbm)):
            if (dr, dq) == (0, 0):
                yield pltpu.make_async_copy(src.at[here], rows.at[slot, kind, span], line_sem.at[there])
            else:
                send = line_send.at[there, kind]
                yield remote(staged.at[kind, here], rows.at[slot, kind, span], line_sem.at[there], send, on_line(dr, dq))

    def tag_line_copy(dr, dq):
        there = place((-dr) % RING, dq)
        return remote(tag_out.at[there], tag_line.at[there], tagp_sem.at[there], tagp_send.at[there], on_line(dr, dq))

    def tag_y_copy(dy):
        there = (-dy) % RING
        return remote(tag_all.at[0], tag_all.at[there], tag_sem.at[0, there], tag_send.at[0, dy], on_plane(dy, 0))

    def tag_z_copy(dz):
        there = (-dz) % RING
        src, dst = tag_all.at[pl.ds(0, RING)], tag_all.at[pl.ds(there * RING, RING)]
        return remote(src, dst, tag_sem.at[1, there], tag_send.at[1, dz], on_plane(0, dz))

    def stage_copy(n):
        return pltpu.make_async_copy((x_hbm, cot_hbm)[n], staged.at[n], local_sem.at[3 + n])

    def hop_copy(name, n, span=None):
        axis, sign, here, part, there = HOPS[name][n]
        if part is not None:
            span = pl.ds(*part)
        src, dst = rows.at[SLOT[here]], rows.at[SLOT[there]]
        if span is not None:
            src, dst = rows.at[SLOT[here], :, span], rows.at[SLOT[there], :, span]
        device = on_plane(sign, 0) if axis == "y" else on_plane(0, sign)
        return remote(src, dst, slot_sem.at[SLOT[there]], hop_send.at[HOP_SEM[name] + n], device)

    def send_hops(*names):
        for name in names:
            for n in range(2):
                hop_copy(name, n).start()

    def send_piece(n):
        half, span = piece(n)
        arrive(rows.at[half, :, span], line_sem.at[n])
        for name in (("y1", "z2"), ("y2", "z1"))[half]:
            for m in range(2):
                hop_copy(name, m, span).start()

    def wait_slots(*keys):
        for key in keys:
            arrive(rows.at[SLOT[key]], slot_sem.at[SLOT[key]])

    def y_copy(half, dz):
        device = on_plane(1 if half == A else 3, 0)
        return remote(ys.at[half, dz], ry.at[half, dz], ry_sem.at[half, dz], ry_send.at[half, dz], device)

    def y_send(*keys):
        for half, dz in keys:
            ys[half, dz] = rgb[OWED_SLOT[(half, 1 if half == A else 3, dz)]].astype(BF16)
        for half, dz in keys:
            y_copy(half, dz).start()

    def relay_copy(half):
        return remote(zs.at[half, 0], zq.at[half], zq_sem.at[half], zq_send.at[half], on_plane(0, 1 if half == A else 3))

    def z_copy(half, dz):
        n = 0 if dz == 1 else 1
        return remote(zs.at[half, 1 + n], zr.at[half, n], zr_sem.at[half, n], zr_send.at[half, n], on_plane(0, dz))

    def home_copy(dr, dq):
        n = place(dr, dq)
        there = place((-dr) % RING, dq)
        src = fs.at[pl.ds(n * CAP, CAP)]
        return remote(src, home.at[cap_rows(me)], home_sem.at[there], home_send.at[n], on_line(dr, dq))

    def total(half, dz):
        arrive(ry.at[half, dz], ry_sem.at[half, dz])
        return rgb[OWED_SLOT[(half, 0, dz)]] + ry[half, dz].astype(F32)

    def make_tags():
        lane = lax.broadcasted_iota(jnp.int32, (8, 128), 1)
        count = jnp.zeros_like(lane)
        for group in range(LINE):
            count = jnp.where(lane // CAP == group, count_smem[0, group], count)
        tags = jnp.where(lane % CAP < count, jnp.broadcast_to(ids_ref[...], (8, 128)), 4).astype(F32)
        for dr, dq in ((0, 0),) + STEPS:
            n = place((-dr) % RING, dq)
            shift = ((n - line_index(dr, dq)) * CAP) % 128
            moved = jnp.where(lane // CAP == n, pltpu.roll(tags, shift, 1), 0.0)
            (tag_line if n == 0 else tag_out)[n] = moved

    def make_gates(slots):
        row = lax.broadcasted_iota(jnp.int32, (HALF, 128), 0)
        lane = lax.broadcasted_iota(jnp.int32, (HALF, 128), 1)
        for n in slots:
            half, dy, dz = ORDER[n]
            tags = tag_all[dz * RING + dy][0:1, :]
            lanes = jnp.zeros_like(tags)
            for task in range(4):
                lanes = jnp.where(tags == float(task), gate_smem[task, blk], lanes)
            picked = jnp.where(lane == row + half * HALF, jnp.broadcast_to(lanes, (HALF, 128)), 0.0)
            gates[n] = jnp.broadcast_to(jnp.sum(picked, axis=1, keepdims=True), (HALF, 128))

    def forward(k):
        four = pl.ds(k * CHUNK, CHUNK)
        span = pl.ds(pl.multiple_of((k % 2) * ROWS, ROWS), ROWS)
        gate = gates[four].reshape(ROWS, 128)
        for n in range(rows.shape[3] // 128):
            cols = pl.ds(n * 128, 128)
            cot = rows[four, 1, :, cols].reshape(ROWS, 128).astype(F32)
            sc[span, cols] = (gate * cot).astype(BF16)

        def body(n, _):
            cols = pl.ds(pl.multiple_of(n * NT, NT), NT)
            pre = jnp.dot(rows[four, 0].reshape(ROWS, rows.shape[3]), w1[:, cols], preferred_element_type=F32)
            back = dot_t(sc[span, :], w2[cols, :])
            sig = 0.5 * jnp.tanh(0.5 * pre) + 0.5
            value = pre * sig
            act[span, cols] = value.astype(BF16)
            pg[span, cols] = (back * (sig + value * (1.0 - sig))).astype(BF16)
            return 0

        lax.fori_loop(0, w1.shape[1] // NT, body, 0)

    def row_grads(k, r):
        span = pl.ds(pl.multiple_of((k % 2) * ROWS, ROWS), ROWS)

        def body(n, _):
            cols = pl.ds(pl.multiple_of(n * RT, RT), RT)
            part = dot_t(pg[span, :], w1[cols, :])
            rgb[pl.ds(r * CHUNK, CHUNK), :, cols] = part.reshape(CHUNK, HALF, RT)
            return 0

        lax.fori_loop(0, w1.shape[0] // RT, body, 0)

    def turn(slots, first, count):
        width = xt.shape[0]
        for n in range(width // 256):
            cols = pl.ds(pl.multiple_of(yhi * width + n * 256, 256), 256)
            xt[pl.ds(n * 256, 256), pl.ds(0, count)] = rows[slots, 0, :, cols].reshape(count, 256).T
        width = actt.shape[0]
        for n in range(width // 256):
            cols = pl.ds(pl.multiple_of(yhi * width + n * 256, 256), 256)
            actt[pl.ds(n * 256, 256), pl.ds(0, count)] = act[pl.ds(first, count), cols].T

    def grads(first, count, last=False):
        here, span = pl.ds(0, count), pl.ds(first, count)

        def add(acc, cols, value):
            value = acc[:, cols] + value
            acc[:, cols] = value * grad_scale if last else value

        def body_in(n, _):
            cols = pl.ds(pl.multiple_of(n * GT_IN, GT_IN), GT_IN)
            add(gin, cols, jnp.dot(xt[:, here], pg[span, cols], preferred_element_type=F32))
            return 0

        def body_out(n, _):
            cols = pl.ds(pl.multiple_of(n * GT_OUT, GT_OUT), GT_OUT)
            add(gout, cols, jnp.dot(actt[:, here], sc[span, cols], preferred_element_type=F32))
            return 0

        lax.fori_loop(0, gin.shape[1] // GT_IN, body_in, 0)
        lax.fori_loop(0, gout.shape[1] // GT_OUT, body_out, 0)

    ids_copy = pltpu.make_async_copy(ids_hbm, ids_ref, local_sem.at[2])
    ids_copy.start()
    for copy in line_copies(0, 0):
        copy.start()
    for n in range(2):
        stage_copy(n).start()
    for n in range(2):
        weight_copy(n).start()

    barrier = pltpu.get_barrier_semaphore()
    around = [(n, 0) for n in range(1, RING)] + [(0, n) for n in range(1, RING)]
    for step in STEPS:
        pl.semaphore_signal(barrier, inc=1, device_id=on_line(*step), device_id_type=MESH)
    for step in around:
        pl.semaphore_signal(barrier, inc=1, device_id=on_plane(*step), device_id_type=MESH)
    ids_copy.wait()
    make_tags()
    for n in range(2):
        stage_copy(n).wait()
    pl.semaphore_wait(barrier, len(STEPS) + len(around))

    for step in STEPS:
        tag_line_copy(*step).start()
    for step in STEPS:
        for copy in line_copies(*step):
            copy.start()

    send_piece(0)
    send_piece(1)
    for n in range(1, LINE):
        arrive(tag_line.at[n], tagp_sem.at[n])
    tags = tag_line[0]
    for n in range(1, LINE):
        tags = tags + tag_line[n]
    tag_all[0] = tags
    for n in range(1, RING):
        tag_y_copy(n).start()
    for n in (2, 4):
        send_piece(n)
    for n in range(1, RING):
        arrive(tag_all.at[n], tag_sem.at[0, n])
    for n in range(1, RING):
        tag_z_copy(n).start()
    for n in (3, 5, 6, 7):
        send_piece(n)

    gin[...] = jnp.zeros_like(gin)
    gout[...] = jnp.zeros_like(gout)
    for n in range(2):
        weight_copy(n).wait()
    for n in range(1, RING):
        arrive(tag_all.at[pl.ds(n * RING, RING)], tag_sem.at[1, n])
    make_gates(range(CHUNK))

    def step(k, _):
        @pl.when(k == 0)
        def _():
            wait_slots((A, 0, 1), (A, 0, 3), (A, 1, 0), (A, 3, 0))
            send_hops("z4", "y3")

        @pl.when(k == 1)
        def _():
            make_gates(range(CHUNK, len(ORDER)))
            wait_slots((B, 0, 1), (B, 0, 3), (B, 3, 0), (B, 1, 0))
            send_hops("y4", "z3", "y5", "z5")

        @pl.when(k == 2)
        def _():
            wait_slots((A, 1, 1), (A, 1, 3), (B, 0, 2))
            send_hops("y6", "z6", "z7")
            wait_slots((B, 3, 1), (B, 1, 1), (A, 2, 0))
            send_hops("z8")

        @pl.when(k == 3)
        def _():
            wait_slots((B, 1, 3))

        @pl.when(k == 4)
        def _():
            wait_slots((A, 0, 2), (A, 1, 2), (A, 3, 1), (A, 3, 3))
            send_hops("z9")
            wait_slots((B, 3, 3), (B, 3, 2))

        @pl.when(k == 6)
        def _():
            wait_slots((A, 3, 2), (B, 2, 0))

        @pl.when(k == 7)
        def _():
            for half in (A, B):
                value = total(half, 0)
                for n in range(2):
                    arrive(zr.at[half, n], zr_sem.at[half, n])
                    value = value + zr[half, n].astype(F32)
                fs[pl.ds(half * HALF, HALF), :] = value.astype(BF16)
            for dr, dq in STEPS:
                home_copy(dr, dq).start()
            home[cap_rows(me), :] = fs[pl.ds(0, CAP), :]
            wait_slots((A, 2, 2), (B, 2, 1), (B, 2, 3), (B, 2, 2))

        forward(k)

        @pl.when((k < 3) | (k == 4))
        def _():
            row_grads(k, k - k // 4)

        @pl.when(k == 2)
        def _():
            y_send((A, 1), (B, 1))
            send_hops("y7")

        @pl.when(k == 4)
        def _():
            y_send((A, 2), (B, 2))
            y_send((A, 3), (B, 3), (A, 0), (B, 0))
            wait_slots((B, 1, 2))
            send_hops("y8", "y9", "y10")

        @pl.when(k == 5)
        def _():
            wait_slots((A, 2, 1), (A, 2, 3))
            send_hops("z10")

        @pl.when(k == 6)
        def _():
            for half, dz in ((A, 3), (B, 1)):
                zs[half, 1 if dz == 1 else 2] = total(half, dz).astype(BF16)
            z_copy(A, 3).start()
            z_copy(B, 1).start()

        @pl.when((k % 2 == 1) & (k < 6))
        def _():
            turn(pl.ds((k - 1) * CHUNK, 2 * CHUNK), 0, PAIR)
            grads(0, PAIR)

        @pl.when(k == 5)
        def _():
            for half in (A, B):
                zs[half, 0] = total(half, 2).astype(BF16)
            for half in (A, B):
                relay_copy(half).start()

        @pl.when(k == 6)
        def _():
            turn(pl.ds(6 * CHUNK, CHUNK), 0, ROWS)
            grads(0, ROWS)
            for half, dz in ((A, 1), (B, 3)):
                arrive(zq.at[half], zq_sem.at[half])
                zs[half, 1 if dz == 1 else 2] = (total(half, dz) + zq[half].astype(F32)).astype(BF16)
            z_copy(A, 1).start()
            z_copy(B, 3).start()

        @pl.when(k == 7)
        def _():
            turn(pl.ds(7 * CHUNK, CHUNK), ROWS, ROWS)
            grads(ROWS, ROWS, last=True)

        return 0

    lax.fori_loop(0, len(ORDER) // CHUNK, step, 0)

    for dr, dq in STEPS:
        arrive(home.at[cap_rows(line_index(dr, dq))], home_sem.at[place(dr, dq)])
    home_ref[...] = home[...]

    for dr, dq in STEPS:
        tag_line_copy(dr, dq).wait_send()
        for copy in line_copies(dr, dq):
            copy.wait_send()
        home_copy(dr, dq).wait_send()
    for n in range(1, RING):
        tag_y_copy(n).wait_send()
        tag_z_copy(n).wait_send()
    for name in HOPS:
        for n in range(2):
            hop_copy(name, n).wait_send()
    for half in (A, B):
        for dz in range(RING):
            y_copy(half, dz).wait_send()
        relay_copy(half).wait_send()
        for dz in (1, 3):
            z_copy(half, dz).wait_send()


def write_out(home_ref, gin_ref, gout_ref, home_hbm, gin_hbm, gout_hbm, home32, sem):
    copies = [pltpu.make_async_copy(gin_ref, gin_hbm, sem.at[0]), pltpu.make_async_copy(gout_ref, gout_hbm, sem.at[1])]
    for copy in copies:
        copy.start()
    home32[...] = home_ref[...].astype(F32)
    copies.append(pltpu.make_async_copy(home32, home_hbm, sem.at[2]))
    copies[2].start()
    for copy in copies:
        copy.wait()


def in_hbm(*arrays):
    return tuple(pltpu.with_memory_space_constraint(array, pltpu.HBM) for array in arrays)


def on_device(inputs, cotangent, task_ids, group_counts, task_gate, w_in, w_out):
    rows, width = inputs.shape
    hidden = w_in.shape[2]
    any_space = pl.BlockSpec(memory_space=pl.ANY)
    hbm = pl.BlockSpec(memory_space=pltpu.HBM)
    smem = pl.BlockSpec(memory_space=pltpu.SMEM)
    vmem = pl.BlockSpec(memory_space=pltpu.VMEM)
    dma = pltpu.SemaphoreType.DMA
    home, gin, gout = pl.pallas_call(
        kernel,
        out_shape=(
            pltpu.VMEM((rows, width), BF16),
            pltpu.VMEM((width // 2, hidden), F32),
            pltpu.VMEM((hidden // 2, width), F32),
        ),
        in_specs=[hbm, hbm, hbm, smem, smem, hbm, hbm],
        out_specs=(vmem,) * 3,
        scratch_shapes=[
            pltpu.VMEM((len(ORDER), 2, HALF, width), BF16),
            pltpu.VMEM((width, hidden), BF16),
            pltpu.VMEM((hidden, width), BF16),
            pltpu.VMEM((PAIR, width), BF16),
            pltpu.VMEM((PAIR, hidden), BF16),
            pltpu.VMEM((PAIR, hidden), BF16),
            pltpu.VMEM((width // 2, PAIR), BF16),
            pltpu.VMEM((hidden // 2, PAIR), BF16),
            pltpu.VMEM((len(ORDER), HALF, 128), F32),
            pltpu.VMEM((LINE, 8, LINE * CAP), F32),
            pltpu.VMEM((LINE, 8, LINE * CAP), F32),
            pltpu.VMEM((RING * RING, 8, LINE * CAP), F32),
            pltpu.VMEM((len(OWED) * CHUNK, HALF, width), F32),
            pltpu.VMEM((2, RING, HALF, width), BF16),
            pltpu.VMEM((2, RING, HALF, width), BF16),
            pltpu.VMEM((2, 3, HALF, width), BF16),
            pltpu.VMEM((2, HALF, width), BF16),
            pltpu.VMEM((2, 2, HALF, width), BF16),
            pltpu.VMEM((2 * HALF, width), BF16),
            pltpu.VMEM((2 * HALF, width), BF16),
            pltpu.VMEM((1, 2 * HALF), jnp.int32),
            pltpu.VMEM((2, rows, width), BF16),
            dma((5,)),
            dma((LINE,)),
            dma((LINE,)),
            dma((LINE,)),
            dma((LINE, 2)),
            dma((2, RING)),
            dma((2, RING)),
            dma((len(ORDER),)),
            dma((2 * len(HOPS),)),
            dma((2, RING)),
            dma((2, RING)),
            dma((2,)),
            dma((2,)),
            dma((2, 2)),
            dma((2, 2)),
            dma((LINE,)),
            dma((LINE,)),
        ],
        compiler_params=pltpu.CompilerParams(
            collective_id=0, has_side_effects=True, vmem_limit_bytes=VMEM_LIMIT
        ),
    )(*in_hbm(inputs, cotangent, task_ids.reshape(1, rows)), group_counts, task_gate, *in_hbm(w_in[0], w_out[0]))
    home, gin, gout = pl.pallas_call(
        write_out,
        out_shape=(
            jax.ShapeDtypeStruct((rows, width), F32),
            jax.ShapeDtypeStruct((width // 2, hidden), F32),
            jax.ShapeDtypeStruct((hidden // 2, width), F32),
        ),
        in_specs=[vmem, any_space, any_space],
        out_specs=(any_space,) * 3,
        scratch_shapes=[pltpu.VMEM((rows, width), F32), dma((3,))],
        compiler_params=pltpu.CompilerParams(vmem_limit_bytes=4 * 1024 * 1024),
    )(home, gin, gout)
    return home, gin[None], gout[None]


def solution(mesh):
    in_specs = (
        P(("blk", "dp"), None),
        P(("blk", "dp"), None),
        P(("blk", "dp")),
        P(("blk", "dp"), None),
        P(),
        P("blk", None, None),
        P("blk", None, None),
    )
    out_specs = (P(("blk", "dp"), None), P("blk", "dp", None), P("blk", "dp", None))
    return jax.shard_map(on_device, mesh=mesh, in_specs=in_specs, out_specs=out_specs, check_vma=False)
```
